256 devices in a mesh: tp: 16 (over z_lo, y), dp: 16 (over z_hi, x, core).
Axes of the slice: x: 4, y: 4, z: 8 (z_hi: 2, z_lo: 4; z = z_hi * 4 + z_lo), core: 2. Of those that a mesh axis runs over, the one named last changes fastest.
Arguments:
- normed: bfloat16 [8192, 4096], P(('dp', 'tp')), may hold values from -6 to 6
- cotangent: bfloat16 [8192, 8192], P('dp', 'tp'), may hold values from -0.52734375 to 0.52734375
- weight_tiles: bfloat16 [2, 2048, 128, 128], P(None, 'tp'), may hold values from -0.09375 to 0.09375
- slot_tile: int32 [2048], replicated, may hold values from 0 to 2047, as said below
Outputs:
- hidden: bfloat16 [8192, 8192], P('dp', 'tp')
- d_normed: bfloat16 [8192, 4096], P(('dp', 'tp'))
- grad_tiles: float32 [2, 2048, 128, 128], P(None, 'tp', 'dp')
The draws below stay inside these ranges and needn't reach their ends.
Inputs may be any that keep to these rules, and one draw needn't show every extreme that they name: `slot_tile`: A permutation of 0 to 2047. Position p belongs to owner p // 128 at slot p % 128. Each owner holds 6 to 10 tiles of the tile columns t * 4 to (t + 1) * 4 - 1 of each index t of tp; in every draw some owner holds exactly 10 for some t.
All inputs are finite; a program needn't handle non-finite values.
Results may differ from the reference program's by a relative error of at most 0.018.
Values may be sent and summed in bfloat16 or wider, within the bound.
A program may use at most 128 MiB of HBM per device.

```python
import jax
import jax.numpy as jnp
from jax import lax

D = 4096
FW = 8192
TILE = 128
TOKENS = 8192
TR = 32
TC = 64
TPC = 4
NTILES = 2048
OWN = 128
N_DP = 16


def tile_layout(key):
    groups = TC // TPC
    owned_count = OWN
    base_count = owned_count // groups
    swing_count = base_count // 4
    key_offset, key_cons, key_owner = jax.random.split(jax.random.fold_in(key, 7), 3)
    offset_draw = jax.random.randint(key_offset, (), 0, groups)
    owner_axis = jnp.arange(groups)[:, None]
    cons_axis = jnp.arange(groups)[None, :]
    phase_step = (cons_axis - owner_axis + offset_draw) % groups
    counts = base_count + swing_count * (1 - 2 * (phase_step % 2))
    list_ends = jnp.cumsum(counts, axis=0)
    starts = list_ends - counts
    rank_ix = jnp.arange(owned_count)
    owner_of = jnp.sum((rank_ix[None, :, None] >= list_ends.T[:, None, :]).astype(jnp.int32), axis=2)
    index_in = rank_ix[None, :] - jnp.take_along_axis(starts.T, owner_of, axis=1)
    local_perm = jax.vmap(lambda sub: jax.random.permutation(sub, owned_count))(jax.random.split(key_cons, groups))
    cons_rows = jnp.broadcast_to(jnp.arange(groups)[:, None], (groups, owned_count))
    tile_row = local_perm // TPC
    tile_col = cons_rows * TPC + local_perm % TPC
    tile_id = (tile_row * TC + tile_col).astype(jnp.int32)
    offsets = jnp.cumsum(counts, axis=1) - counts
    pre_slot = offsets[owner_of, cons_rows] + index_in
    shuffles = jax.vmap(lambda sub: jax.random.permutation(sub, owned_count))(jax.random.split(key_owner, groups))
    slot_ix = shuffles[owner_of, pre_slot].astype(jnp.int32)
    slot_table = jnp.zeros((NTILES,), jnp.int32).at[(owner_of * owned_count + slot_ix).reshape(-1)].set(tile_id.reshape(-1))
    return slot_table


def draw_slot_tile(key, part):
    return tile_layout(key)


def shard_levels(stream_key, shape, cuts, low, high):
    factor_of, own = 1.0, jax.random.fold_in(stream_key, 6)
    for dim, shards_of in cuts:
        steps = jnp.exp(jax.random.uniform(jax.random.fold_in(own, dim), (shards_of,), jnp.float32, low / len(cuts), high / len(cuts)))
        factor_of = factor_of * jnp.repeat(steps, shape[dim] // shards_of).reshape([-1 if axis == dim else 1 for axis in range(len(shape))])
    return factor_of


def scatter_about(stream_key, shape, scale, reach, shards=(), kind=jnp.bfloat16):
    drawn = scale * jax.random.normal(stream_key, shape, jnp.float32)
    if shards:
        drawn = drawn * shard_levels(stream_key, shape, shards, -0.22, 0.18)
    return jnp.clip(drawn, -reach, reach).astype(kind)


def setup_inputs(seed: int = 0) -> dict:
    splits = jax.random.split(jax.random.key(seed), 5)
    normed = scatter_about(splits[0], (TOKENS, D), 1.0, 6.0, ((0, 256),))
    cotangent = scatter_about(splits[1], (TOKENS, FW), (8.0 / TOKENS ** 0.5), 0.52734375, ((0, 16), (1, 16)))
    weight_tiles = scatter_about(splits[2], (2, NTILES, TILE, TILE), D ** -0.5, 0.09375, ((1, 16),))
    slot_tile = draw_slot_tile(jax.random.fold_in(splits[4], 71), 0)
    return {"normed": normed, "cotangent": cotangent, "weight_tiles": weight_tiles, "slot_tile": slot_tile}


def reference(normed, cotangent, weight_tiles, slot_tile):
    by_number = jnp.zeros_like(weight_tiles).at[:, slot_tile].set(weight_tiles)
    weights = by_number.reshape(2, TR, TC, TILE, TILE).transpose(0, 1, 3, 2, 4).reshape(2, D, FW)
    gate_proj = jnp.dot(normed, weights[0], preferred_element_type=jnp.float32)
    up_proj = jnp.dot(normed, weights[1], preferred_element_type=jnp.float32)
    sigmoid_gate = jax.nn.sigmoid(gate_proj)
    act_gate = gate_proj * sigmoid_gate
    hidden = (act_gate * up_proj).astype(jnp.bfloat16)
    cot_full = cotangent.astype(jnp.float32)
    grad_gate = (cot_full * up_proj * (sigmoid_gate * (1.0 + gate_proj * (1.0 - sigmoid_gate)))).astype(jnp.bfloat16)
    grad_up = (cot_full * act_gate).astype(jnp.bfloat16)
    d_normed = (jnp.dot(grad_gate, weights[0].T, preferred_element_type=jnp.float32)
                + jnp.dot(grad_up, weights[1].T, preferred_element_type=jnp.float32)).astype(jnp.bfloat16)

    def replica(running, group_block):
        rows_in, rows_gate, rows_up = group_block
        part_gate = jnp.dot(rows_in.T, rows_gate, preferred_element_type=jnp.float32).astype(jnp.bfloat16)
        part_up = jnp.dot(rows_in.T, rows_up, preferred_element_type=jnp.float32).astype(jnp.bfloat16)
        stacked = lax.optimization_barrier(jnp.stack([part_gate, part_up]))
        return running + stacked.astype(jnp.float32), None

    start_sum = jnp.zeros((2, D, FW), jnp.float32)
    summed, _ = lax.scan(replica, start_sum, (normed.reshape(N_DP, -1, D), grad_gate.reshape(N_DP, -1, FW), grad_up.reshape(N_DP, -1, FW)))
    grad_tiled = summed.reshape(2, TR, TILE, TC, TILE).transpose(0, 1, 3, 2, 4).reshape(2, TR * TC, TILE, TILE)
    grad_tiles = grad_tiled[:, slot_tile]
    return hidden, d_normed, grad_tiles
```

```python
import jax
import jax.numpy as jnp
from jax import lax
from jax.experimental import pallas as pl
from jax.experimental.pallas import tpu as pltpu
from jax.sharding import Mesh
from jax.sharding import PartitionSpec as P

D = 4096
FW = 8192
TILE = 128
TC = FW // TILE
OWNERS = 16
OWN = 128
CPD = TC // OWNERS
RANKS = 10
TOK = 32
GROUP = 512
AXES = ("zl", "y", "zh", "x", "c")
MESH = pl.DeviceIdType.MESH
BF = jnp.bfloat16
F32 = jnp.float32
DZ = (1, 7, 2, 6, 0)


def index_lists(slot_tile, me):
    tiles = slot_tile.reshape(OWNERS, OWN)
    target = tiles % TC // CPD
    seq = jnp.arange(OWN, dtype=jnp.int32)
    ahead = seq[None, None, :] < seq[None, :, None]
    same = target[:, :, None] == target[:, None, :]
    rank = jnp.sum((same & ahead).astype(jnp.int32), axis=2)
    owners = jnp.arange(OWNERS, dtype=jnp.int32)
    ranks = jnp.arange(RANKS, dtype=jnp.int32)
    my_target = lax.dynamic_index_in_dim(target, me, 0, keepdims=False)
    my_rank = lax.dynamic_index_in_dim(rank, me, 0, keepdims=False)
    my_code = my_target * RANKS + my_rank
    codes = jnp.arange(OWNERS * RANKS, dtype=jnp.int32)
    pick = jnp.sum(jnp.where(my_code[None, :] == codes[:, None], seq[None, :], 0), axis=1)
    mine = target == me
    place = tiles // TC * CPD + tiles % TC - me * CPD
    source = owners[:, None] * RANKS + rank
    inverse = jnp.sum(
        jnp.where(mine[None] & (place[None] == seq[:, None, None]), source[None], 0), axis=(1, 2)
    )
    grad_pick = jnp.sum(
        jnp.where(mine[:, None, :] & (rank[:, None, :] == ranks[None, :, None]), place[:, None, :], 0),
        axis=2,
    ).reshape(-1)
    return pick, inverse, grad_pick, my_code


def kernel(
    pick_ref, inv_ref, gpick_ref, ginv_ref, tok_hbm, cot_hbm, own_hbm,
    hid_hbm, dn_hbm, gt_hbm,
    own, outg, arrv, xs, ws, cot, hid, acc, grads, term, yfar, ynear, zrecv, dnout,
    part, precv, xfar, xnear, fsum, gout, garr, give, gres,
    ld, a_s, a_r, tz_s, tz_r, tn_s, tn_r, tf_s, tf_r, wn_s, wn_r, wf_s, wf_r, wd_s, wd_r,
    pd_s, pd_r, xf_s, xf_r, xn_s, xn_r, yf_s, yf_r, yn_s, yn_r, zr_s, zr_r, g_s, g_r, q_s, q_r,
):
    zl, y, zh, x, c = (lax.axis_index(a) for a in AXES)
    z = zh * 4 + zl
    me = zl * 4 + y

    def dev(dz=0, dy=0, dx=0, dc=0):
        zz = lax.rem(z + dz, 8)
        return (
            lax.rem(zz, 4), lax.rem(y + dy, 4), lax.div(zz, 4), lax.rem(x + dx, 4), lax.rem(c + dc, 2),
        )

    def rcopy(src, dst, ss, rs, to):
        return pltpu.make_async_remote_copy(
            src_ref=src, dst_ref=dst, send_sem=ss, recv_sem=rs, device_id=to, device_id_type=MESH
        )

    sends = []

    def send(src, dst, ss, rs, to):
        copy = rcopy(src, dst, ss, rs, to)
        copy.start()
        sends.append(copy)

    def recv(dst, ss, rs):
        rcopy(dst, dst, ss, rs, dev(dc=1)).wait_recv()

    band = x * 2 + c
    load_own = pltpu.make_async_copy(
        own_hbm.at[:, :, pl.ds(pl.multiple_of(band * 16, 16), 16), :], own, ld.at[0]
    )
    load_own.start()
    load_tok = pltpu.make_async_copy(tok_hbm, xs.at[zl, y], ld.at[1])
    load_tok.start()
    load_cot = pltpu.make_async_copy(cot_hbm, cot, ld.at[2])
    load_cot.start()

    barrier = pltpu.get_barrier_semaphore()

    @pl.loop(1, 32)
    def _(j):
        dz, dy = lax.div(j, 4), lax.rem(j, 4)
        pl.semaphore_signal(barrier, inc=1, device_id=dev(dz, dy), device_id_type=MESH)

    for to in (dev(dx=1), dev(dx=3), dev(dc=1)):
        pl.semaphore_signal(barrier, inc=1, device_id=to, device_id_type=MESH)

    load_own.wait()

    def pick_into(dst, t):
        @pl.loop(0, RANKS)
        def _(k):
            slot = pick_ref[t * RANKS + k]
            for m in range(2):
                dst[t * RANKS + k, m] = own[m, slot]

    pick_into(arrv, me)
    pl.semaphore_wait(barrier, 34)

    def tile_message(dz, dy, ref, far_side):
        zz = lax.rem(z + (8 - dz if far_side else dz), 8)
        other = lax.rem(zz, 4) * 4 + lax.rem(y + (4 - dy if far_side else dy), 4)
        rows = pl.ds(other * RANKS, RANKS)
        if dz == 2:
            return ref.at[rows, 0]
        if dz == 6:
            return ref.at[rows, 1]
        return ref.at[rows]

    mine_rows = pl.ds(me * RANKS, RANKS)

    def landing(dz, ref):
        if dz == 2:
            return ref.at[mine_rows, 0]
        if dz == 6:
            return ref.at[mine_rows, 1]
        return ref.at[mine_rows]

    for i, dz in enumerate(DZ):
        for dy in range(4):
            if dz == 0 and dy == 0:
                continue
            if dz != 6:
                zz = lax.rem(z + dz, 8)
                pick_into(outg, lax.rem(zz, 4) * 4 + lax.rem(y + dy, 4))
            n = i * 4 + dy
            send(tile_message(dz, dy, outg, False), landing(dz, arrv), a_s.at[n], a_r.at[n], dev(dz, dy))

    load_tok.wait()
    for j in range(1, 4):
        to = (lax.rem(zl + j, 4), y, zh, x, c)
        send(xs.at[zl, y], xs.at[zl, y], tz_s.at[j - 1], tz_r.at[j - 1], to)

    def near_tokens(q):
        zq = lax.rem(zl + 4 - q, 4)
        for way, dy in ((0, 1), (1, 3)):
            send(xs.at[zq, y], xs.at[zq, y], tn_s.at[q, way], tn_r.at[q, way], dev(dy=dy))

    def far_tokens(q):
        zq = lax.rem(zl + 4 - q, 4)
        for way, dy in ((0, 1), (1, 3)):
            src = lax.rem(y + 4 - dy, 4)
            recv(xs.at[zq, src], tn_s.at[q, way], tn_r.at[q, way])
            half = pl.ds(16 * way, 16)
            send(xs.at[zq, src, half], xs.at[zq, src, half], tf_s.at[q, way], tf_r.at[q, way], dev(dy=dy))

    def last_tokens(q):
        zq, src = lax.rem(zl + 4 - q, 4), lax.rem(y + 2, 4)
        for way in range(2):
            recv(xs.at[zq, src, pl.ds(16 * way, 16)], tf_s.at[q, way], tf_r.at[q, way])

    near_tokens(0)

    for i, dz in enumerate(DZ):
        for dy in range(4):
            if dz == 0 and dy == 0:
                continue
            n = i * 4 + dy
            recv(tile_message(dz, dy, arrv, True), a_s.at[n], a_r.at[n])

    @pl.loop(0, D // TILE)
    def _(r):
        for col in range(CPD):
            src = inv_ref[r * CPD + col]
            for m in range(2):
                ws[m, r, band, :, col * TILE : (col + 1) * TILE] = arrv[src, m]

    for m in range(2):
        for way in range(2):
            mm = m if way == 0 else 1 - m
            send(
                ws.at[mm, :, band], ws.at[mm, :, band], wn_s.at[mm, way], wn_r.at[mm, way],
                dev(dx=1 if way == 0 else 3),
            )
    for m in range(2):
        send(ws.at[m, :, band], ws.at[m, :, band], wd_s.at[m], wd_r.at[m], dev(dc=1))

    for q in range(1, 4):
        recv(xs.at[lax.rem(zl + 4 - q, 4), y], tz_s.at[q - 1], tz_r.at[q - 1])
        near_tokens(q)

    far_tokens(0)

    def side_band(way, core):
        return lax.rem(x + (3 if way == 0 else 1), 4) * 2 + core

    def near_weights(m, way, n, forward):
        b = side_band(way, c)
        block = ws.at[m, :, b]
        recv(block, wn_s.at[m, way], wn_r.at[m, way])
        if forward:
            send(block, block, wf_s.at[way], wf_r.at[way], dev(dx=1 if way == 0 else 3))
        send(block, block, wd_s.at[n], wd_r.at[n], dev(dc=1))

    near_weights(0, 0, 2, True)
    near_weights(1, 1, 3, True)
    far_tokens(1)
    far_tokens(2)
    near_weights(1, 0, 4, False)
    near_weights(0, 1, 5, False)
    far_tokens(3)
    far_x = lax.rem(x + 2, 4) * 2
    for way in range(2):
        block = ws.at[way, :, far_x + c]
        recv(block, wf_s.at[way], wf_r.at[way])
        send(block, block, wd_s.at[6 + way], wd_r.at[6 + way], dev(dc=1))
    for q in range(4):
        last_tokens(q)
    other = 1 - c
    for m in range(2):
        recv(ws.at[m, :, x * 2 + other], wd_s.at[m], wd_r.at[m])
        recv(ws.at[m, :, far_x + other], wd_s.at[6 + m], wd_r.at[6 + m])
    for n, m, way in ((2, 0, 0), (3, 1, 1), (4, 1, 0), (5, 0, 1)):
        recv(ws.at[m, :, side_band(way, other)], wd_s.at[n], wd_r.at[n])

    @pl.loop(0, 4)
    def _(k):
        cols = pl.ds(pl.multiple_of(k * 1024, 1024), 1024)
        a = xs[:, :, :, cols].reshape(GROUP, 1024)
        for m in range(2):
            w = ws[m, pl.ds(k * 8, 8)].reshape(1024, GROUP)
            v = jnp.dot(a, w, preferred_element_type=F32)

            @pl.when(k == 0)
            def _():
                acc[m] = v

            @pl.when(k > 0)
            def _():
                acc[m] += v

    load_cot.wait()

    @pl.loop(0, 16)
    def _(i):
        rows = pl.ds(pl.multiple_of(i * 32, 32), 32)
        gate, up = acc[0, rows], acc[1, rows]
        s = jax.nn.sigmoid(gate)
        act = gate * s
        ct = cot[rows].astype(F32)
        hid[rows] = (act * up).astype(BF)
        grads[rows, :GROUP] = (ct * up * (s * (1.0 + gate * (1.0 - s)))).astype(BF)
        grads[rows, GROUP:] = (ct * act).astype(BF)

    store_hid = pltpu.make_async_copy(hid, hid_hbm, ld.at[3])
    store_hid.start()

    @pl.loop(0, 8)
    def _(d):
        cols = pl.ds(pl.multiple_of(d * 512, 512), 512)
        a = xs[:, :, :, cols].reshape(GROUP, 512)
        v = lax.dot_general(a, grads[...], (((0,), (0,)), ((), ())), preferred_element_type=F32)
        v = v.astype(BF).reshape(4, 2, 4, 16, 1024)
        half, row = lax.div(d, 4), lax.rem(d, 4) * 4
        for m in range(2):
            for xx in range(4):
                for col in range(CPD):
                    lo = m * GROUP + col * TILE
                    part[m, xx, half, pl.ds(row, 4), col] = v[:, :, xx, :, lo : lo + TILE]

    ring = lambda pos: (lax.rem(pos + 2, 4), lax.rem(pos + 1, 4), lax.rem(pos + 3, 4), pos)
    xt = ring(x)
    for i in range(4):
        send(part.at[other, xt[i]], precv.at[xt[i]], pd_s.at[i], pd_r.at[i], dev(dc=1))

    @pl.loop(0, 8)
    def _(d):
        v = None
        for m in range(2):
            w = ws[m, pl.ds(d * 4, 4)].reshape(GROUP, GROUP)
            g = grads[:, m * GROUP : (m + 1) * GROUP]
            t = lax.dot_general(g, w, (((1,), (1,)), ((), ())), preferred_element_type=F32)
            v = t if v is None else v + t
        v = v.astype(BF).reshape(2, 2, 4, TOK, 512)
        cols = pl.ds(pl.multiple_of(d * 512, 512), 512)
        for yy in range(4):
            term[yy, :, :, :, cols] = v[:, :, yy]

    yt = ring(y)

    def ring_far(a, t, far, ss, rs, to):
        for way in range(2):
            send(a.at[t[0], way], far.at[way], ss.at[way], rs.at[way], to[way])

    def ring_free(a, t, near, ss, rs, to):
        for way in range(2):
            h = 1 - way
            send(a.at[t[1 + way], h], near.at[way, h], ss.at[way, h], rs.at[way, h], to[way])

    def ring_sum(a, t, far, near, fs, fr, ss, rs, to, add):
        for way in range(2):
            recv(far.at[way], fs.at[way], fr.at[way])
            add(t[1 + way], way, far)
            send(a.at[t[1 + way], way], near.at[way, way], ss.at[way, way], rs.at[way, way], to[way])

    y_to = (dev(dy=1), dev(dy=3))
    x_to = (dev(dx=1), dev(dx=3))
    ring_far(term, yt, yfar, yf_s, yf_r, y_to)
    ring_free(term, yt, ynear, yn_s, yn_r, y_to)

    mine = part.at[c]

    def add_partner(t):
        for h in range(2):
            @pl.loop(0, 16)
            def _(r):
                mine[t, h, r] = (mine[t, h, r].astype(F32) + precv[t, h, r].astype(F32)).astype(BF)

    for i in range(4):
        recv(precv.at[xt[i]], pd_s.at[i], pd_r.at[i])
        add_partner(xt[i])
        if i == 0:
            ring_far(mine, xt, xfar, xf_s, xf_r, x_to)
        if i == 2:
            ring_free(mine, xt, xnear, xn_s, xn_r, x_to)

    def add_term(t, way, far):
        @pl.loop(0, 8)
        def _(i):
            cols = pl.ds(pl.multiple_of(i * 512, 512), 512)
            here = term[t, way, :, :, cols].astype(F32)
            term[t, way, :, :, cols] = (here + far[way, :, :, cols].astype(F32)).astype(BF)

    def add_part(t, way, far):
        @pl.loop(0, 16)
        def _(r):
            mine[t, way, r] = (mine[t, way, r].astype(F32) + far[way, r].astype(F32)).astype(BF)

    ring_sum(term, yt, yfar, ynear, yf_s, yf_r, yn_s, yn_r, y_to, add_term)
    ring_sum(mine, xt, xfar, xnear, xf_s, xf_r, xn_s, xn_r, x_to, add_part)

    for way in range(2):
        for h in range(2):
            recv(ynear.at[way, h], yn_s.at[way, h], yn_r.at[way, h])
    for h in range(2):
        @pl.loop(0, 8)
        def _(i):
            cols = pl.ds(pl.multiple_of(i * 512, 512), 512)
            total = term[y, h, :, :, cols].astype(F32)
            for way in range(2):
                total += ynear[way, h, :, :, cols].astype(F32)
            term[y, h, :, :, cols] = total.astype(BF)

    for j in range(1, 4):
        zt = lax.rem(zl + j, 4)
        send(
            term.at[y, lax.div(zt, 2), lax.rem(zt, 2)], zrecv.at[j - 1], zr_s.at[j - 1], zr_r.at[j - 1],
            (zt, y, zh, x, c),
        )

    for way in range(2):
        for h in range(2):
            recv(xnear.at[way, h], xn_s.at[way, h], xn_r.at[way, h])
    for h in range(2):
        @pl.loop(0, 16)
        def _(r):
            total = mine[x, h, r].astype(F32)
            for way in range(2):
                total += xnear[way, h, r].astype(F32)
            total = total.astype(BF)
            for col in range(CPD):
                fsum[(h * 16 + r) * CPD + col] = total[col]

    def pick_grads(dz, dy):
        zz = lax.rem(z + dz, 8)
        owner, high = lax.rem(zz, 4) * 4 + lax.rem(y + dy, 4), lax.div(zz, 4)

        @pl.loop(0, RANKS)
        def _(k):
            tile = gpick_ref[owner * RANKS + k]
            gout[high, owner * RANKS + k] = fsum[tile, high]

        return owner, high

    for dz in (4, 3, 5, 2, 6, 1, 7, 0):
        for dy in (2, 1, 3, 0):
            if dz == 0 and dy == 0:
                continue
            owner, high = pick_grads(dz, dy)
            n = dz * 4 + dy
            send(
                gout.at[high, pl.ds(owner * RANKS, RANKS)], garr.at[zh, mine_rows],
                g_s.at[n], g_r.at[n], dev(dz, dy),
            )

    @pl.loop(0, RANKS)
    def _(k):
        garr[zh, me * RANKS + k] = fsum[gpick_ref[me * RANKS + k], zh]

    for j in range(1, 4):
        recv(zrecv.at[j - 1], zr_s.at[j - 1], zr_r.at[j - 1])

    @pl.loop(0, 8)
    def _(i):
        cols = pl.ds(pl.multiple_of(i * 512, 512), 512)
        total = term[y, lax.div(zl, 2), lax.rem(zl, 2), :, cols].astype(F32)
        for j in range(3):
            total += zrecv[j, :, cols].astype(F32)
        dnout[:, cols] = total.astype(BF)

    store_dn = pltpu.make_async_copy(dnout, dn_hbm, ld.at[4])
    store_dn.start()

    for dz in range(8):
        for dy in range(4):
            if dz == 0 and dy == 0:
                continue
            zz = lax.rem(z + 8 - dz, 8)
            source, high = lax.rem(zz, 4) * 4 + lax.rem(y + 4 - dy, 4), lax.div(zz, 4)
            n = dz * 4 + dy
            recv(garr.at[high, pl.ds(source * RANKS, RANKS)], g_s.at[n], g_r.at[n])

    @pl.loop(0, OWN, unroll=4)
    def _(s):
        src = ginv_ref[s]
        total = garr[0, src].astype(F32) + garr[1, src].astype(F32)
        low, high = total[:8], total[8:]
        gres[c, s] = jnp.where(c == 0, low, high)
        give[s] = jnp.where(c == 0, high, low)

    swap = rcopy(give, gres.at[c], q_s.at[0], q_r.at[0], dev(dc=1))
    swap.start()
    sends.append(swap)
    store_a = pltpu.make_async_copy(gres.at[c], gt_hbm.at[c], ld.at[5])
    store_a.start()
    recv(gres.at[other], q_s.at[0], q_r.at[0])
    store_b = pltpu.make_async_copy(gres.at[other], gt_hbm.at[other], ld.at[6])
    store_b.start()
    for copy in sends:
        copy.wait_send()
    for copy in (store_hid, store_dn, store_a, store_b):
        copy.wait()


def step(normed, cotangent, weight_tiles, slot_tile):
    me = lax.axis_index(("zl", "y"))
    lists = index_lists(slot_tile, me)
    dma = pltpu.SemaphoreType.DMA
    scratch = [
        pltpu.VMEM((2, OWN, 16, TILE), BF),
        pltpu.VMEM((160, 2, 16, TILE), BF),
        pltpu.VMEM((160, 2, 16, TILE), BF),
        pltpu.VMEM((4, 4, TOK, D), BF),
        pltpu.VMEM((2, 32, 8, 16, GROUP), BF),
        pltpu.VMEM((GROUP, GROUP), BF),
        pltpu.VMEM((GROUP, GROUP), BF),
        pltpu.VMEM((2, GROUP, GROUP), F32),
        pltpu.VMEM((GROUP, 2 * GROUP), BF),
        pltpu.VMEM((4, 2, 2, TOK, D), BF),
        pltpu.VMEM((2, 2, TOK, D), BF),
        pltpu.VMEM((2, 2, 2, TOK, D), BF),
        pltpu.VMEM((3, TOK, D), BF),
        pltpu.VMEM((TOK, D), BF),
        pltpu.VMEM((2, 4, 2, 16, 4, 2, 16, TILE), BF),
        pltpu.VMEM((4, 2, 16, 4, 2, 16, TILE), BF),
        pltpu.VMEM((2, 16, 4, 2, 16, TILE), BF),
        pltpu.VMEM((2, 2, 16, 4, 2, 16, TILE), BF),
        pltpu.VMEM((OWN, 2, 16, TILE), BF),
        pltpu.VMEM((2, 160, 16, TILE), BF),
        pltpu.VMEM((2, 160, 16, TILE), BF),
        pltpu.VMEM((OWN, 8, TILE), F32),
        pltpu.VMEM((2, OWN, 8, TILE), F32),
        dma((7,)),
    ]
    for shape in (
        (20,), (3,), (4, 2), (4, 2), (2, 2), (2,), (8,), (4,), (2,), (2, 2), (2,), (2, 2), (3,), (32,), (1,),
    ):
        scratch += [dma(shape), dma(shape)]
    smem, anywhere = pl.BlockSpec(memory_space=pltpu.SMEM), pl.BlockSpec(memory_space=pl.ANY)
    return pl.pallas_call(
        kernel,
        out_shape=(
            jax.ShapeDtypeStruct((GROUP, GROUP), BF),
            jax.ShapeDtypeStruct((TOK, D), BF),
            jax.ShapeDtypeStruct((2, OWN, 8, TILE), F32),
        ),
        in_specs=[smem] * 4 + [anywhere] * 3,
        out_specs=[anywhere] * 3,
        scratch_shapes=scratch,
        compiler_params=pltpu.CompilerParams(
            collective_id=0, has_side_effects=True, vmem_limit_bytes=67_043_328
        ),
        name="gated_pair",
    )(*lists, normed, cotangent, weight_tiles)


def solution(mesh):
    finer = Mesh(mesh.devices.reshape(4, 4, 2, 4, 2), AXES)
    tp, dp = ("zl", "y"), ("zh", "x", "c")
    return jax.shard_map(
        step,
        mesh=finer,
        in_specs=(P(dp + tp, None), P(dp, tp), P(None, tp, None, None), P()),
        out_specs=(P(dp, tp), P(dp + tp, None), P(None, tp, dp, None)),
        check_vma=False,
    )
```

```python
import jax
import jax.numpy as jnp
from jax import lax
from jax.experimental import pallas as pl
from jax.experimental.pallas import tpu as pltpu
from jax.sharding import Mesh
from jax.sharding import PartitionSpec as P

D = 4096
FW = 8192
TILE = 128
TC = FW // TILE
OWNERS = 16
OWN = 128
CPD = TC // OWNERS
RANKS = 10
TOK = 32
GROUP = 512
AXES = ("zl", "y", "zh", "x", "c")
MESH = pl.DeviceIdType.MESH
BF = jnp.bfloat16
F32 = jnp.float32
SENT = tuple(
    [(m, dz, dy) for m in range(2) for dz in (2, 6, 1, 7, 0) for dy in range(4)
     if (dz or dy) and (dz not in (2, 6) or (dz == 2) == ((dy < 2) == (m == 0)))]
)
STAGES = 4
COLS = D // STAGES


def kernel(
    tiles_ref, tok_hbm, cot_hbm, own_hbm,
    hid_hbm, dn_hbm, gt_hbm,
    keys, rows, lists, own, outg, arrv_a, arrv_b, xs, ws, cot, hid, acc, grads, term, yfar, ynear, zrecv, dnout,
    part, precv, xfar, xnear, fsum, gout, garr, give, gres,
    ld, a_s, a_r, tz_s, tz_r, tn_s, tn_r, tf_s, tf_r, wn_s, wn_r, wf_s, wf_r, wd_s, wd_r,
    pd_s, pd_r, xf_s, xf_r, xn_s, xn_r, yf_s, yf_r, yn_s, yn_r, zr_s, zr_r, g_s, g_r, q_s, q_r,
):
    zl, y, zh, x, c = (lax.axis_index(a) for a in AXES)
    z = zh * 4 + zl
    me = zl * 4 + y
    other = 1 - c

    def dev(dz=0, dy=0, dx=0, dc=0):
        zz = lax.rem(z + dz, 8)
        return (
            lax.rem(zz, 4), lax.rem(y + dy, 4), lax.div(zz, 4), lax.rem(x + dx, 4), lax.rem(c + dc, 2),
        )

    def rcopy(src, dst, ss, rs, to):
        return pltpu.make_async_remote_copy(
            src_ref=src, dst_ref=dst, send_sem=ss, recv_sem=rs, device_id=to, device_id_type=MESH
        )

    arrv = (arrv_a, arrv_b)
    scopes = []

    def phase(name):
        if scopes:
            scopes.pop().__exit__(None, None, None)
        if name:
            scopes.append(jax.named_scope(name))
            scopes[-1].__enter__()

    sends = []

    def send(src, dst, ss, rs, to):
        copy = rcopy(src, dst, ss, rs, to)
        copy.start()
        sends.append(copy)

    def recv(dst, ss, rs):
        rcopy(dst, dst, ss, rs, dev(dc=1)).wait_recv()

    phase("p00_load")
    band = x * 2 + c
    load_own = pltpu.make_async_copy(
        own_hbm.at[:, :, pl.ds(pl.multiple_of(band * 16, 16), 16), :], own, ld.at[0]
    )
    load_tok = pltpu.make_async_copy(tok_hbm, xs.at[zl, y], ld.at[1])
    load_cot = pltpu.make_async_copy(cot_hbm, cot, ld.at[2])
    load_tok.start()
    load_own.start()

    barrier = pltpu.get_barrier_semaphore()

    @pl.loop(1, 32)
    def _(j):
        dz, dy = lax.div(j, 4), lax.rem(j, 4)
        pl.semaphore_signal(barrier, inc=1, device_id=dev(dz, dy), device_id_type=MESH)

    for to in (dev(dx=1), dev(dx=3), dev(dc=1)):
        pl.semaphore_signal(barrier, inc=1, device_id=to, device_id_type=MESH)

    phase("p01_lists")
    tiles = tiles_ref[...]
    lane = lax.broadcasted_iota(jnp.int32, (OWNERS, OWN), 1)
    owner_id = lax.broadcasted_iota(jnp.int32, (OWNERS, OWN), 0)
    target = lax.shift_right_logical(tiles & (TC - 1), 2)
    place = lax.shift_right_logical(tiles, 6) * CPD + (tiles & (TC - 1)) - me * CPD
    rank = jnp.zeros_like(tiles)
    for t in range(OWNERS):
        hit = target == t
        count = jnp.where(hit, 1, 0)
        for step_of in (1, 2, 4, 8, 16, 32, 64):
            count += jnp.where(lane >= step_of, pltpu.roll(count, step_of, 1), 0)
        rank = jnp.where(hit, count - 1, rank)
    mine = target == me
    last = OWNERS * RANKS - 1
    source = jnp.minimum(owner_id * RANKS + rank, last)
    code = jnp.minimum(target * RANKS + rank, last)
    my_code = jnp.max(jnp.where(owner_id == me, code, 0), axis=0, keepdims=True)
    keys[0:16] = jnp.where(mine, place, -1)
    keys[16:32] = source
    keys[32:48] = jnp.where(mine, source, -1)
    keys[48:64] = place
    keys[64:128] = jnp.broadcast_to(my_code, (64, OWN))
    keys[...] = keys[...].T
    wide = lax.broadcasted_iota(jnp.int32, (8, 2 * OWN), 1)
    seq = lax.broadcasted_iota(jnp.int32, (8, 2 * OWN), 0)

    def fold(i, sums):
        col = keys[pl.ds(pl.multiple_of(i * 8, 8), 8)]
        inverse, gpick, pick = sums
        for o in range(OWNERS):
            hit_a = jnp.where(col[:, o : o + 1] == wide, col[:, 16 + o : 17 + o], 0)
            hit_b = jnp.where(col[:, 32 + o : 33 + o] == wide, col[:, 48 + o : 49 + o], 0)
            inverse, gpick = jnp.maximum(inverse, hit_a), jnp.maximum(gpick, hit_b)
        pick = jnp.maximum(pick, jnp.where(col[:, 64:65] == wide, seq + i * 8, 0))
        return inverse, gpick, pick

    zero = jnp.zeros((8, 2 * OWN), jnp.int32)
    inverse, gpick, pick = lax.fori_loop(0, 16, fold, (zero, zero, zero))
    rows[0:1] = jnp.max(pick, axis=0, keepdims=True)
    rows[1:2] = jnp.max(inverse, axis=0, keepdims=True)
    rows[2:3] = jnp.max(gpick, axis=0, keepdims=True)
    rows[3:4, :OWN] = my_code
    rows[3:4, OWN:] = my_code
    load_lists = pltpu.make_async_copy(rows, lists, ld.at[7])
    load_lists.start()

    phase("p02_barrier")
    pl.semaphore_wait(barrier, 34)
    load_cot.start()
    load_tok.wait()

    def zq_of(q):
        return lax.rem(zl + 4 - q, 4)

    def near_tokens(q):
        block = xs.at[zq_of(q), y]
        for way, dy in ((0, 1), (1, 3)):
            send(block, block, tn_s.at[q, way], tn_r.at[q, way], dev(dy=dy))

    def far_tokens(q):
        for way, dy in ((0, 1), (1, 3)):
            src = lax.rem(y + 4 - dy, 4)
            recv(xs.at[zq_of(q), src], tn_s.at[q, way], tn_r.at[q, way])
            half = xs.at[zq_of(q), src, pl.ds(16 * way, 16)]
            send(half, half, tf_s.at[q, way], tf_r.at[q, way], dev(dy=dy))

    def last_tokens(q):
        src = lax.rem(y + 2, 4)
        for way in range(2):
            recv(xs.at[zq_of(q), src, pl.ds(16 * way, 16)], tf_s.at[q, way], tf_r.at[q, way])

    near_tokens(0)

    phase("p03_pick_send")
    load_lists.wait()
    load_own.wait()
    my_rows = pl.ds(me * RANKS, RANKS)

    def tp_of(dz, dy):
        return lax.rem(lax.rem(z + dz, 8), 4) * 4 + lax.rem(y + dy, 4)

    def pick_into(dst, m, t):
        @pl.loop(0, RANKS)
        def _(k):
            dst[t * RANKS + k] = own[m, lists[0, t * RANKS + k]]

    for n, (m, dz, dy) in enumerate(SENT):
        t = tp_of(dz, dy)
        pick_into(outg.at[m], m, t)
        send(outg.at[m, pl.ds(t * RANKS, RANKS)], arrv[m].at[my_rows], a_s.at[n], a_r.at[n], dev(dz, dy))
    for m in range(2):
        pick_into(arrv[m], m, me)

    phase("p04_tokz")
    for j in (1, 3, 2):
        to = (lax.rem(zl + j, 4), y, zh, x, c)
        send(xs.at[zl, y], xs.at[zl, y], tz_s.at[j - 1], tz_r.at[j - 1], to)

    def side_band(way, core):
        return lax.rem(x + (3 if way == 0 else 1), 4) * 2 + core

    far_x = lax.rem(x + 2, 4) * 2
    x_to = (dev(dx=1), dev(dx=3))
    y_to = (dev(dy=1), dev(dy=3))

    def own_weights(m):
        phase(f"p05_wait_a2a{m}")
        for n, (mm, dz, dy) in enumerate(SENT):
            if mm == m:
                t = tp_of(8 - dz, 4 - dy)
                recv(arrv[m].at[pl.ds(t * RANKS, RANKS)], a_s.at[n], a_r.at[n])
        phase(f"p06_place{m}")

        @pl.loop(0, D // TILE)
        def _(r):
            for col in range(CPD):
                ws[m, r, band, :, col * TILE : (col + 1) * TILE] = arrv[m][lists[1, r * CPD + col]]

        block = ws.at[m, :, band]
        for way in range(2):
            send(block, block, wn_s.at[m, way], wn_r.at[m, way], x_to[way])
        send(block, block, wd_s.at[m, 0], wd_r.at[m, 0], dev(dc=1))

    def near_weights(m):
        phase(f"p09_nearw{m}")
        for way in range(2):
            block = ws.at[m, :, side_band(way, c)]
            recv(block, wn_s.at[m, way], wn_r.at[m, way])
            half = ws.at[m, pl.ds(16 * way, 16), side_band(way, c)]
            send(half, half, wf_s.at[m, way], wf_r.at[m, way], x_to[way])
            send(block, block, wd_s.at[m, 1 + way], wd_r.at[m, 1 + way], dev(dc=1))

    def far_weights(m):
        phase(f"p13_farw{m}")
        for way in range(2):
            half = ws.at[m, pl.ds(16 * way, 16), far_x + c]
            recv(half, wf_s.at[m, way], wf_r.at[m, way])
            send(half, half, wd_s.at[m, 3 + way], wd_r.at[m, 3 + way], dev(dc=1))

    def partner_weights(m):
        phase(f"p15_d2d{m}")
        recv(ws.at[m, :, x * 2 + other], wd_s.at[m, 0], wd_r.at[m, 0])
        for way in range(2):
            recv(ws.at[m, :, side_band(way, other)], wd_s.at[m, 1 + way], wd_r.at[m, 1 + way])
            recv(ws.at[m, pl.ds(16 * way, 16), far_x + other], wd_s.at[m, 3 + way], wd_r.at[m, 3 + way])

    def tokens_z(q):
        phase(f"p07_tokz{q}")
        recv(xs.at[zq_of(q), y], tz_s.at[q - 1], tz_r.at[q - 1])
        near_tokens(q)

    own_weights(0)
    own_weights(1)
    phase("p08_far0")
    far_tokens(0)
    tokens_z(1)
    tokens_z(3)
    near_weights(0)
    tokens_z(2)
    phase("p10_far1")
    far_tokens(1)
    near_weights(1)
    phase("p10_far3")
    far_tokens(3)
    far_weights(0)
    phase("p10_far2")
    far_tokens(2)
    far_weights(1)
    partner_weights(0)
    partner_weights(1)
    phase("p14_lasttok")
    for q in (0, 1, 3, 2):
        last_tokens(q)

    phase("p16_fwd")

    @pl.loop(0, 4)
    def _(k):
        cols = pl.ds(pl.multiple_of(k * 1024, 1024), 1024)
        a = xs[:, :, :, cols].reshape(GROUP, 1024)
        for m in range(2):
            w = ws[m, pl.ds(k * 8, 8)].reshape(1024, GROUP)
            v = jnp.dot(a, w, preferred_element_type=F32)

            @pl.when(k == 0)
            def _():
                acc[m] = v

            @pl.when(k > 0)
            def _():
                acc[m] += v

    phase("p17_elem")
    load_cot.wait()

    @pl.loop(0, 16)
    def _(i):
        rows_of = pl.ds(pl.multiple_of(i * 32, 32), 32)
        gate, up = acc[0, rows_of], acc[1, rows_of]
        s = jax.nn.sigmoid(gate)
        act = gate * s
        ct = cot[rows_of].astype(F32)
        hid[rows_of] = (act * up).astype(BF)
        grads[rows_of, :GROUP] = (ct * up * (s * (1.0 + gate * (1.0 - s)))).astype(BF)
        grads[rows_of, GROUP:] = (ct * act).astype(BF)

    store_hid = pltpu.make_async_copy(hid, hid_hbm, ld.at[3])
    store_hid.start()

    def share(st):
        phase(f"p20_dn{st}")

        @pl.loop(0, COLS // 512)
        def _(d):
            v = None
            for m in range(2):
                w = ws[m, pl.ds(st * (COLS // TILE) + d * 4, 4)].reshape(GROUP, GROUP)
                g = grads[:, m * GROUP : (m + 1) * GROUP]
                t = lax.dot_general(g, w, (((1,), (1,)), ((), ())), preferred_element_type=F32)
                v = t if v is None else v + t
            v = v.astype(BF).reshape(2, 2, 4, TOK, 512)
            cols = pl.ds(pl.multiple_of(d * 512, 512), 512)
            for yy in range(4):
                term[st, yy, :, :, :, cols] = v[:, :, yy]

    def ring(pos):
        return lax.rem(pos + 2, 4), lax.rem(pos + 1, 4), lax.rem(pos + 3, 4), pos

    xt, yt = ring(x), ring(y)

    def ring_open(a, t, far, near, fs, fr, ss, rs, to):
        for way in range(2):
            send(a(t[0], way), far.at[way], fs.at[way], fr.at[way], to[way])
        for way in range(2):
            h = 1 - way
            send(a(t[1 + way], h), near.at[way, h], ss.at[way, h], rs.at[way, h], to[way])

    def ring_pass(a, t, far, near, fs, fr, ss, rs, to, add):
        for way in range(2):
            recv(far.at[way], fs.at[way], fr.at[way])
            add(t[1 + way], way)
            send(a(t[1 + way], way), near.at[way, way], ss.at[way, way], rs.at[way, way], to[way])

    def ring_close(near, ss, rs):
        for way in range(2):
            for h in range(2):
                recv(near.at[way, h], ss.at[way, h], rs.at[way, h])

    def y_args(st):
        a = lambda t, h: term.at[st, t, h]
        return a, yt, yfar.at[st], ynear.at[st], yf_s.at[st], yf_r.at[st], yn_s.at[st], yn_r.at[st], y_to

    def y_open(st):
        ring_open(*y_args(st))

    def y_pass(st):
        phase(f"p23_ypass{st}")

        def add(t, way):
            here = term[st, t, way].astype(F32)
            term[st, t, way] = (here + yfar[st, way].astype(F32)).astype(BF)

        ring_pass(*y_args(st), add)

    def y_close(st):
        phase(f"p25_yclose{st}")
        ring_close(ynear.at[st], yn_s.at[st], yn_r.at[st])
        for h in range(2):
            total = term[st, y, h].astype(F32)
            for way in range(2):
                total += ynear[st, way, h].astype(F32)
            term[st, y, h] = total.astype(BF)
        for j in range(1, 4):
            zt = lax.rem(zl + j, 4)
            send(
                term.at[st, y, lax.div(zt, 2), lax.rem(zt, 2)], zrecv.at[st, j - 1],
                zr_s.at[st, j - 1], zr_r.at[st, j - 1], (zt, y, zh, x, c),
            )

    highs = (1 - zh, zh)
    mat = part.at[c]

    def partner_sum(k):
        phase(f"p22_partner{k}")
        for i in range(4):
            recv(precv.at[xt[i], highs[k]], pd_s.at[k, i], pd_r.at[k, i])
            for h in range(2):

                @pl.loop(0, 4)
                def _(r):
                    at = (xt[i], highs[k], h, pl.ds(r * 4, 4))
                    mat[at] = (mat[at].astype(F32) + precv[at].astype(F32)).astype(BF)

    def x_args(k):
        a = lambda t, h: mat.at[t, highs[k], h]
        return a, xt, xfar.at[k], xnear.at[k], xf_s.at[k], xf_r.at[k], xn_s.at[k], xn_r.at[k], x_to

    def x_open(k):
        ring_open(*x_args(k))

    def x_pass(k):
        phase(f"p24_xpass{k}")

        def add(t, way):
            @pl.loop(0, 4)
            def _(r):
                rs = pl.ds(r * 4, 4)
                at = (t, highs[k], way, rs)
                mat[at] = (mat[at].astype(F32) + xfar[k, way, rs].astype(F32)).astype(BF)

        ring_pass(*x_args(k), add)

    def x_close(k):
        phase(f"p27_xclose{k}")
        ring_close(xnear.at[k], xn_s.at[k], xn_r.at[k])
        for h in range(2):

            @pl.loop(0, 16)
            def _(r):
                total = mat[x, highs[k], h, r].astype(F32)
                for way in range(2):
                    total += xnear[k, way, h, r].astype(F32)
                fsum[k, pl.ds((h * 16 + r) * CPD, CPD)] = total.astype(BF)

        for dzl in (0, 1, 3, 2):
            for dy in (2, 1, 3, 0):
                owner = lax.rem(zl + dzl, 4) * 4 + lax.rem(y + dy, 4)
                here = k == 1 and dzl == 0 and dy == 0

                @pl.loop(0, RANKS)
                def _(i):
                    tile = fsum[k, lists[2, owner * RANKS + i]]
                    if here:
                        garr[zh, owner * RANKS + i] = tile
                    else:
                        gout[k, owner * RANKS + i] = tile

                if not here:
                    n = dzl * 4 + dy
                    to = (lax.rem(zl + dzl, 4), lax.rem(y + dy, 4), highs[k], x, c)
                    send(
                        gout.at[k, pl.ds(owner * RANKS, RANKS)], garr.at[zh, my_rows],
                        g_s.at[k, n], g_r.at[k, n], to,
                    )

    share(0)
    y_open(0)

    phase("p18_dw")

    @pl.loop(0, 8)
    def _(d):
        cols = pl.ds(pl.multiple_of(d * 512, 512), 512)
        a = xs[:, :, :, cols].reshape(GROUP, 512)
        v = lax.dot_general(a, grads[...], (((0,), (0,)), ((), ())), preferred_element_type=F32)
        v = v.astype(BF).reshape(4, 2, 4, 16, 1024)
        half, row = lax.div(d, 4), lax.rem(d, 4) * 4
        for m in range(2):
            for xx in range(4):
                for col in range(CPD):
                    lo = m * GROUP + col * TILE
                    for high in range(2):
                        part[m, xx, high, half, pl.ds(row, 4), col] = v[:, high, xx, :, lo : lo + TILE]

    for k in range(2):
        for i in range(4):
            send(
                part.at[other, xt[i], highs[k]], precv.at[xt[i], highs[k]],
                pd_s.at[k, i], pd_r.at[k, i], dev(dc=1),
            )

    y_pass(0)
    share(1)
    y_open(1)
    partner_sum(0)
    x_open(0)
    share(2)
    share(3)
    partner_sum(1)
    y_pass(1)
    y_open(2)
    y_close(0)
    x_pass(0)
    x_open(1)
    y_close(1)
    y_pass(2)
    y_open(3)
    y_close(2)
    x_close(0)
    y_pass(3)
    x_pass(1)
    y_close(3)
    x_close(1)

    phase("p30_zrecv")
    for st in range(STAGES):
        for j in range(1, 4):
            recv(zrecv.at[st, j - 1], zr_s.at[st, j - 1], zr_r.at[st, j - 1])
        total = term[st, y, lax.div(zl, 2), lax.rem(zl, 2)].astype(F32)
        for j in range(3):
            total += zrecv[st, j].astype(F32)
        dnout[:, st * COLS : (st + 1) * COLS] = total.astype(BF)

    store_dn = pltpu.make_async_copy(dnout, dn_hbm, ld.at[4])
    store_dn.start()

    for k in range(2):
        phase(f"p31_ga2a{k}")
        for n in range(16):
            if k == 1 and n == 0:
                continue
            dzl, dy = divmod(n, 4)
            src = lax.rem(zl + 4 - dzl, 4) * 4 + lax.rem(y + 4 - dy, 4)
            recv(garr.at[highs[k], pl.ds(src * RANKS, RANKS)], g_s.at[k, n], g_r.at[k, n])

    phase("p32_final")

    @pl.loop(0, OWN, unroll=4)
    def _(s):
        src = lists[3, s]
        total = garr[0, src].astype(F32) + garr[1, src].astype(F32)
        low, high = total[:8], total[8:]
        gres[c, s] = jnp.where(c == 0, low, high)
        give[s] = jnp.where(c == 0, high, low)

    phase("p33_swap")
    send(give, gres.at[c], q_s.at[0], q_r.at[0], dev(dc=1))
    store_a = pltpu.make_async_copy(gres.at[c], gt_hbm.at[c], ld.at[5])
    store_a.start()
    recv(gres.at[other], q_s.at[0], q_r.at[0])
    store_b = pltpu.make_async_copy(gres.at[other], gt_hbm.at[other], ld.at[6])
    store_b.start()
    phase("p34_drain")
    for copy in sends:
        copy.wait_send()
    for copy in (store_hid, store_dn, store_a, store_b):
        copy.wait()
    phase(None)


def step(normed, cotangent, weight_tiles, slot_tile):
    dma = pltpu.SemaphoreType.DMA
    scratch = [
        pltpu.VMEM((OWN, OWN), jnp.int32),
        pltpu.VMEM((8, 2 * OWN), jnp.int32),
        pltpu.SMEM((8, 2 * OWN), jnp.int32),
        pltpu.VMEM((2, OWN, 16, TILE), BF),
        pltpu.VMEM((2, 160, 16, TILE), BF),
        pltpu.VMEM((160, 16, TILE), BF),
        pltpu.VMEM((160, 16, TILE), BF),
        pltpu.VMEM((4, 4, TOK, D), BF),
        pltpu.VMEM((2, 32, 8, 16, GROUP), BF),
        pltpu.VMEM((GROUP, GROUP), BF),
        pltpu.VMEM((GROUP, GROUP), BF),
        pltpu.VMEM((2, GROUP, GROUP), F32),
        pltpu.VMEM((GROUP, 2 * GROUP), BF),
        pltpu.VMEM((STAGES, 4, 2, 2, TOK, COLS), BF),
        pltpu.VMEM((STAGES, 2, 2, TOK, COLS), BF),
        pltpu.VMEM((STAGES, 2, 2, 2, TOK, COLS), BF),
        pltpu.VMEM((STAGES, 3, TOK, COLS), BF),
        pltpu.VMEM((TOK, D), BF),
        pltpu.VMEM((2, 4, 2, 2, 16, 4, 16, TILE), BF),
        pltpu.VMEM((4, 2, 2, 16, 4, 16, TILE), BF),
        pltpu.VMEM((2, 2, 16, 4, 16, TILE), BF),
        pltpu.VMEM((2, 2, 2, 16, 4, 16, TILE), BF),
        pltpu.VMEM((2, OWN, 16, TILE), BF),
        pltpu.VMEM((2, 160, 16, TILE), BF),
        pltpu.VMEM((2, 160, 16, TILE), BF),
        pltpu.VMEM((OWN, 8, TILE), F32),
        pltpu.VMEM((2, OWN, 8, TILE), F32),
        dma((8,)),
    ]
    for shape in (
        (len(SENT),), (3,), (4, 2), (4, 2), (2, 2), (2, 2), (2, 5), (2, 4), (2, 2), (2, 2, 2),
        (STAGES, 2), (STAGES, 2, 2), (STAGES, 3), (2, 16), (1,),
    ):
        scratch += [dma(shape), dma(shape)]
    anywhere = pl.BlockSpec(memory_space=pl.ANY)
    return pl.pallas_call(
        kernel,
        out_shape=(
            jax.ShapeDtypeStruct((GROUP, GROUP), BF),
            jax.ShapeDtypeStruct((TOK, D), BF),
            jax.ShapeDtypeStruct((2, OWN, 8, TILE), F32),
        ),
        in_specs=[pl.BlockSpec(memory_space=pltpu.VMEM)] + [anywhere] * 3,
        out_specs=[anywhere] * 3,
        scratch_shapes=scratch,
        compiler_params=pltpu.CompilerParams(
            collective_id=0, has_side_effects=True, vmem_limit_bytes=67_043_328
        ),
        name="gated_pair",
    )(slot_tile.reshape(OWNERS, OWN), normed, cotangent, weight_tiles)


def solution(mesh):
    finer = Mesh(mesh.devices.reshape(4, 4, 2, 4, 2), AXES)
    tp, dp = ("zl", "y"), ("zh", "x", "c")
    return jax.shard_map(
        step,
        mesh=finer,
        in_specs=(P(dp + tp, None), P(dp, tp), P(None, tp, None, None), P()),
        out_specs=(P(dp, tp), P(dp + tp, None), P(None, tp, dp, None)),
        check_vma=False,
    )
```

```python
import jax
import jax.numpy as jnp
from jax import lax
from jax.experimental import pallas as pl
from jax.experimental.pallas import tpu as pltpu
from jax.sharding import Mesh
from jax.sharding import PartitionSpec as P

D = 4096
FW = 8192
TILE = 128
TC = FW // TILE
OWNERS = 16
OWN = 128
CPD = TC // OWNERS
RANKS = 10
TOK = 32
GROUP = 512
AXES = ("zl", "y", "zh", "x", "c")
MESH = pl.DeviceIdType.MESH
BF = jnp.bfloat16
F32 = jnp.float32
SENT = tuple(
    [(m, dz, dy) for m in range(2) for dz in (2, 6, 1, 7, 0) for dy in range(4)
     if (dz or dy) and (dz not in (2, 6) or (dz == 2) == ((dy < 2) == (m == 0)))]
)
STAGES = 4
COLS = D // STAGES


def kernel(
    tiles_ref, tok_hbm, cot_hbm, own_hbm,
    hid_hbm, dn_hbm, gt_hbm,
    keys, rows, lists, own, outg, arrv_a, arrv_b, xs, ws, cot, hid, acc, grads, term, yfar, ynear, zpair, zcross, dnout,
    part, precv, xfar, xnear, fsum, gout, garr, give, gres,
    ld, a_s, a_r, tz_s, tz_r, tn_s, tn_r, tf_s, tf_r, wn_s, wn_r, wf_s, wf_r, wd_s, wd_r,
    pd_s, pd_r, xf_s, xf_r, xn_s, xn_r, yf_s, yf_r, yn_s, yn_r, zr_s, zr_r, g_s, g_r, q_s, q_r,
):
    zl, y, zh, x, c = (lax.axis_index(a) for a in AXES)
    z = zh * 4 + zl
    me = zl * 4 + y
    other = 1 - c

    def dev(dz=0, dy=0, dx=0, dc=0):
        zz = lax.rem(z + dz, 8)
        return (
            lax.rem(zz, 4), lax.rem(y + dy, 4), lax.div(zz, 4), lax.rem(x + dx, 4), lax.rem(c + dc, 2),
        )

    def rcopy(src, dst, ss, rs, to):
        return pltpu.make_async_remote_copy(
            src_ref=src, dst_ref=dst, send_sem=ss, recv_sem=rs, device_id=to, device_id_type=MESH
        )

    arrv = (arrv_a, arrv_b)
    scopes = []

    def phase(name):
        if scopes:
            scopes.pop().__exit__(None, None, None)
        if name:
            scopes.append(jax.named_scope(name))
            scopes[-1].__enter__()

    sends = []

    def send(src, dst, ss, rs, to):
        copy = rcopy(src, dst, ss, rs, to)
        copy.start()
        sends.append(copy)

    def recv(dst, ss, rs):
        rcopy(dst, dst, ss, rs, dev(dc=1)).wait_recv()

    phase("p00_load")
    band = x * 2 + c
    load_own = pltpu.make_async_copy(
        own_hbm.at[:, :, pl.ds(pl.multiple_of(band * 16, 16), 16), :], own, ld.at[0]
    )
    load_tok = pltpu.make_async_copy(tok_hbm, xs.at[zl, y], ld.at[1])
    load_cot = pltpu.make_async_copy(cot_hbm, cot, ld.at[2])
    load_tok.start()
    load_own.start()

    barrier = pltpu.get_barrier_semaphore()

    @pl.loop(1, 32)
    def _(j):
        dz, dy = lax.div(j, 4), lax.rem(j, 4)
        pl.semaphore_signal(barrier, inc=1, device_id=dev(dz, dy), device_id_type=MESH)

    for to in (dev(dx=1), dev(dx=3), dev(dc=1)):
        pl.semaphore_signal(barrier, inc=1, device_id=to, device_id_type=MESH)

    phase("p01_lists")
    tiles = tiles_ref[...]
    lane = lax.broadcasted_iota(jnp.int32, (OWNERS, OWN), 1)
    owner_id = lax.broadcasted_iota(jnp.int32, (OWNERS, OWN), 0)
    target = lax.shift_right_logical(tiles & (TC - 1), 2)
    place = lax.shift_right_logical(tiles, 6) * CPD + (tiles & (TC - 1)) - me * CPD
    shift = (target & 7) * 4
    one = lax.shift_left(jnp.ones_like(tiles), shift)
    count = [jnp.where(target < 8, one, 0), jnp.where(target < 8, 0, one)]
    for step_of in (1, 2, 4, 8, 16, 32, 64):
        count = [v + jnp.where(lane >= step_of, pltpu.roll(v, step_of, 1), 0) for v in count]
    count = jnp.where(target < 8, count[0], count[1])
    rank = jnp.maximum((lax.shift_right_logical(count, shift) & 15) - 1, 0)
    mine = target == me
    last = OWNERS * RANKS - 1
    source = jnp.minimum(owner_id * RANKS + rank, last)
    code = jnp.minimum(target * RANKS + rank, last)
    my_code = jnp.max(jnp.where(owner_id == me, code, 0), axis=0, keepdims=True)
    key_a, key_b = jnp.where(mine, place, -1), jnp.where(mine, source, -1)
    codes = lax.broadcasted_iota(jnp.int32, (OWNERS * RANKS, OWN), 0)
    spot = codes[:OWN]
    inverse, gpick = jnp.zeros_like(spot), jnp.zeros_like(codes)
    for o in range(OWNERS):
        row = slice(o, o + 1)
        inverse = jnp.maximum(inverse, jnp.where(key_a[row] == spot, source[row], 0))
        gpick = jnp.maximum(gpick, jnp.where(key_b[row] == codes, place[row], 0))
    wide = lax.broadcasted_iota(jnp.int32, codes.shape, 1)
    pick = jnp.max(jnp.where(my_code == codes, wide, 0), axis=1, keepdims=True)
    inverse = jnp.max(inverse, axis=1, keepdims=True)
    gpick = jnp.max(gpick, axis=1, keepdims=True)
    columns = jnp.where(wide == 0, pick, jnp.where(wide == 2, gpick, 0))
    keys[0:OWN] = jnp.where(wide[:OWN] == 1, inverse, columns[:OWN])
    keys[OWN : OWNERS * RANKS] = columns[OWN:]
    keys[OWNERS * RANKS :] = jnp.zeros((2 * OWN - OWNERS * RANKS, OWN), jnp.int32)
    rows[:, :OWN] = keys[:OWN].T[:8]
    rows[:, OWN:] = keys[OWN:].T[:8]
    rows[3:4, :OWN] = my_code
    load_lists = pltpu.make_async_copy(rows, lists, ld.at[7])
    load_lists.start()

    load_own.wait()
    load_lists.wait()
    my_rows = pl.ds(me * RANKS, RANKS)

    def tp_of(dz, dy):
        return lax.rem(lax.rem(z + dz, 8), 4) * 4 + lax.rem(y + dy, 4)

    def pick_tiles(m):
        @pl.loop(0, OWNERS)
        def _(t):
            for k in range(RANKS):
                outg[m, t * RANKS + k] = own[m, lists[0, t * RANKS + k]]

    def send_tiles(m):
        for n, (mm, dz, dy) in enumerate(SENT):
            if mm == m:
                rows_of = pl.ds(tp_of(dz, dy) * RANKS, RANKS)
                send(outg.at[m, rows_of], arrv[m].at[my_rows], a_s.at[n], a_r.at[n], dev(dz, dy))

    phase("p02_pick0")
    pick_tiles(0)
    phase("p02_barrier")
    pl.semaphore_wait(barrier, 34)
    phase("p03_pick_send")
    send_tiles(0)
    pick_tiles(1)
    send_tiles(1)
    load_cot.start()
    load_tok.wait()

    pair = zl + 1 - 2 * lax.rem(zl, 2)
    cross = lax.rem(zl + 2, 4)

    def zq_of(q):
        return (zl, pair, cross, 3 - zl)[q]

    def at_z(to):
        return (to, y, zh, x, c)

    def near_tokens(q):
        for part_of in range(2):
            for way in range(2):
                h = way if part_of == 0 else 1 - way
                block = xs.at[zq_of(q), y, pl.ds(16 * h, 16)]
                send(block, block, tn_s.at[q, way, h], tn_r.at[q, way, h], y_to[way])

    def far_tokens(q):
        phase(f"p08_far{q}")
        for way in range(2):
            src = lax.rem(y + (3 if way == 0 else 1), 4)
            half = xs.at[zq_of(q), src, pl.ds(16 * way, 16)]
            recv(half, tn_s.at[q, way, way], tn_r.at[q, way, way])
            send(half, half, tf_s.at[q, way], tf_r.at[q, way], y_to[way])

    def last_tokens(q):
        phase(f"p14_last{q}")
        for way in range(2):
            src, h = lax.rem(y + (3 if way == 0 else 1), 4), 1 - way
            recv(xs.at[zq_of(q), src, pl.ds(16 * h, 16)], tn_s.at[q, way, h], tn_r.at[q, way, h])
            recv(xs.at[zq_of(q), lax.rem(y + 2, 4), pl.ds(16 * way, 16)], tf_s.at[q, way], tf_r.at[q, way])

    x_to = (dev(dx=1), dev(dx=3))
    y_to = (dev(dy=1), dev(dy=3))
    near_tokens(0)

    for m in range(2):
        for k in range(RANKS):
            arrv[m][me * RANKS + k] = own[m, lists[0, me * RANKS + k]]

    phase("p04_tokz")
    for i, to in enumerate((pair, cross)):
        send(xs.at[zl, y], xs.at[zl, y], tz_s.at[i], tz_r.at[i], at_z(to))

    def side_band(way, core):
        return lax.rem(x + (3 if way == 0 else 1), 4) * 2 + core

    far_x = lax.rem(x + 2, 4) * 2

    def own_weights(m):
        phase(f"p05_wait_a2a{m}")
        for n, (mm, dz, dy) in enumerate(SENT):
            if mm == m:
                t = tp_of(8 - dz, 4 - dy)
                recv(arrv[m].at[pl.ds(t * RANKS, RANKS)], a_s.at[n], a_r.at[n])
        phase(f"p06_place{m}")

        @pl.loop(0, D // TILE)
        def _(r):
            for col in range(CPD):
                ws[m, r, band, :, col * TILE : (col + 1) * TILE] = arrv[m][lists[1, r * CPD + col]]

        block = ws.at[m, :, band]
        for way in range(2):
            send(block, block, wn_s.at[m, way], wn_r.at[m, way], x_to[way])
        send(block, block, wd_s.at[m, 0], wd_r.at[m, 0], dev(dc=1))

    def near_weights(m):
        phase(f"p09_nearw{m}")
        for way in range(2):
            block = ws.at[m, :, side_band(way, c)]
            recv(block, wn_s.at[m, way], wn_r.at[m, way])
            half = ws.at[m, pl.ds(16 * way, 16), side_band(way, c)]
            send(half, half, wf_s.at[m, way], wf_r.at[m, way], x_to[way])
            send(block, block, wd_s.at[m, 1 + way], wd_r.at[m, 1 + way], dev(dc=1))

    def far_weights(m):
        phase(f"p13_farw{m}")
        for way in range(2):
            half = ws.at[m, pl.ds(16 * way, 16), far_x + c]
            recv(half, wf_s.at[m, way], wf_r.at[m, way])
            send(half, half, wd_s.at[m, 3 + way], wd_r.at[m, 3 + way], dev(dc=1))

    def partner_weights(m):
        phase(f"p15_d2d{m}")
        recv(ws.at[m, :, x * 2 + other], wd_s.at[m, 0], wd_r.at[m, 0])
        for way in range(2):
            recv(ws.at[m, :, side_band(way, other)], wd_s.at[m, 1 + way], wd_r.at[m, 1 + way])
            recv(ws.at[m, pl.ds(16 * way, 16), far_x + other], wd_s.at[m, 3 + way], wd_r.at[m, 3 + way])

    def tokens_z(q):
        phase(f"p07_tokz{q}")
        block = xs.at[zq_of(q), y]
        recv(block, tz_s.at[q - 1], tz_r.at[q - 1])
        if q == 2:
            send(block, block, tz_s.at[2], tz_r.at[2], at_z(pair))
        near_tokens(q)

    own_weights(0)
    own_weights(1)
    near_weights(0)
    far_tokens(0)
    tokens_z(1)
    tokens_z(2)
    far_tokens(1)
    tokens_z(3)
    near_weights(1)
    far_tokens(2)
    far_weights(0)
    far_tokens(3)
    far_weights(1)
    last_tokens(0)
    last_tokens(1)
    partner_weights(0)
    partner_weights(1)

    def forward(qa, qb):
        phase(f"p16_fwd{qa}")
        za, zb = zq_of(qa), zq_of(qb)

        @pl.loop(0, 4)
        def _(k):
            cols = pl.ds(pl.multiple_of(k * 1024, 1024), 1024)
            a = jnp.concatenate([xs[zz, :, :, cols].reshape(128, 1024) for zz in (za, zb)], axis=0)
            for m in range(2):
                w = ws[m, pl.ds(k * 8, 8)].reshape(1024, GROUP)
                v = jnp.dot(a, w, preferred_element_type=F32)

                @pl.when(k == 0)
                def _():
                    acc[m, za], acc[m, zb] = v[:128], v[128:]

                @pl.when(k > 0)
                def _():
                    acc[m, za] += v[:128]
                    acc[m, zb] += v[128:]

    forward(0, 1)
    last_tokens(2)
    last_tokens(3)
    forward(2, 3)
    phase("p17_elem")
    load_cot.wait()

    @pl.loop(0, 16)
    def _(i):
        rows_of = pl.ds(pl.multiple_of(i * 32, 32), 32)
        at = (lax.div(i, 4), pl.ds(pl.multiple_of(lax.rem(i, 4) * 32, 32), 32))
        gate, up = acc[0, *at], acc[1, *at]
        s = jax.nn.sigmoid(gate)
        act = gate * s
        ct = cot[rows_of].astype(F32)
        hid[rows_of] = (act * up).astype(BF)
        grads[rows_of, :GROUP] = (ct * up * (s * (1.0 + gate * (1.0 - s)))).astype(BF)
        grads[rows_of, GROUP:] = (ct * act).astype(BF)

    store_hid = pltpu.make_async_copy(hid, hid_hbm, ld.at[3])
    store_hid.start()

    def share(st):
        phase(f"p20_dn{st}")

        @pl.loop(0, COLS // 512)
        def _(d):
            v = None
            for m in range(2):
                w = ws[m, pl.ds(st * (COLS // TILE) + d * 4, 4)].reshape(GROUP, GROUP)
                g = grads[:, m * GROUP : (m + 1) * GROUP]
                t = lax.dot_general(g, w, (((1,), (1,)), ((), ())), preferred_element_type=F32)
                v = t if v is None else v + t
            v = v.astype(BF).reshape(2, 2, 4, TOK, 512)
            cols = pl.ds(pl.multiple_of(d * 512, 512), 512)
            for yy in range(4):
                term[st, yy, :, :, :, cols] = v[:, :, yy]

    def ring(pos):
        return lax.rem(pos + 2, 4), lax.rem(pos + 1, 4), lax.rem(pos + 3, 4), pos

    xt, yt = ring(x), ring(y)

    def ring_open(a, t, far, near, fs, fr, ss, rs, to):
        for way in range(2):
            send(a(t[0], way), far.at[way], fs.at[way], fr.at[way], to[way])
        for way in range(2):
            h = 1 - way
            send(a(t[1 + way], h), near.at[way, h], ss.at[way, h], rs.at[way, h], to[way])

    def ring_pass(a, t, far, near, fs, fr, ss, rs, to, add):
        for way in range(2):
            recv(far.at[way], fs.at[way], fr.at[way])
            add(t[1 + way], way)
            send(a(t[1 + way], way), near.at[way, way], ss.at[way, way], rs.at[way, way], to[way])

    def ring_close(near, ss, rs):
        for way in range(2):
            for h in range(2):
                recv(near.at[way, h], ss.at[way, h], rs.at[way, h])

    def y_args(st):
        a = lambda t, h: term.at[st, t, h]
        return a, yt, yfar.at[st], ynear.at[st], yf_s.at[st], yf_r.at[st], yn_s.at[st], yn_r.at[st], y_to

    def y_open(st):
        ring_open(*y_args(st))

    def y_pass(st):
        phase(f"p23_ypass{st}")

        def add(t, way):
            here = term[st, t, way].astype(F32)
            term[st, t, way] = (here + yfar[st, way].astype(F32)).astype(BF)

        ring_pass(*y_args(st), add)

    def y_close(st):
        phase(f"p25_yclose{st}")
        ring_close(ynear.at[st], yn_s.at[st], yn_r.at[st])
        for h in range(2):
            total = term[st, y, h].astype(F32)
            for way in range(2):
                total += ynear[st, way, h].astype(F32)
            term[st, y, h] = total.astype(BF)
        send(
            term.at[st, y, :, lax.rem(pair, 2)], zpair.at[st], zr_s.at[st, 0], zr_r.at[st, 0], at_z(pair)
        )

    high_z, low_z = lax.div(zl, 2), lax.rem(zl, 2)

    def z_pass(st):
        phase(f"p26_zpass{st}")
        recv(zpair.at[st], zr_s.at[st, 0], zr_r.at[st, 0])
        here = term[st, y, 1 - high_z, low_z].astype(F32)
        term[st, y, 1 - high_z, low_z] = (here + zpair[st, 1 - high_z].astype(F32)).astype(BF)
        send(
            term.at[st, y, 1 - high_z, low_z], zcross.at[st], zr_s.at[st, 1], zr_r.at[st, 1], at_z(cross)
        )

    highs = (1 - zh, zh)
    mat = part.at[c]

    def partner_send(k, h):
        for i in range(4):
            send(
                part.at[other, xt[i], highs[k], h], precv.at[xt[i], highs[k], h],
                pd_s.at[k, i, h], pd_r.at[k, i, h], dev(dc=1),
            )

    def partner_sum(k, h):
        phase(f"p22_partner{k}{h}")
        for i in range(4):
            recv(precv.at[xt[i], highs[k], h], pd_s.at[k, i, h], pd_r.at[k, i, h])

            @pl.loop(0, 4)
            def _(r):
                at = (xt[i], highs[k], h, pl.ds(r * 4, 4))
                mat[at] = (mat[at].astype(F32) + precv[at].astype(F32)).astype(BF)

    def x_far(k, way):
        send(mat.at[xt[0], highs[k], way], xfar.at[k, way], xf_s.at[k, way], xf_r.at[k, way], x_to[way])

    def x_near(k, way, h):
        send(
            mat.at[xt[1 + way], highs[k], h], xnear.at[k, way, h], xn_s.at[k, way, h], xn_r.at[k, way, h],
            x_to[way],
        )

    def x_pass(k, way):
        phase(f"p24_xpass{k}{way}")
        recv(xfar.at[k, way], xf_s.at[k, way], xf_r.at[k, way])

        @pl.loop(0, 4)
        def _(r):
            rs = pl.ds(r * 4, 4)
            at = (xt[1 + way], highs[k], way, rs)
            mat[at] = (mat[at].astype(F32) + xfar[k, way, rs].astype(F32)).astype(BF)

        x_near(k, way, way)

    def x_close(k):
        phase(f"p27_xclose{k}")
        ring_close(xnear.at[k], xn_s.at[k], xn_r.at[k])
        for h in range(2):

            @pl.loop(0, 16)
            def _(r):
                total = mat[x, highs[k], h, r].astype(F32)
                for way in range(2):
                    total += xnear[k, way, h, r].astype(F32)
                fsum[k, pl.ds((h * 16 + r) * CPD, CPD)] = total.astype(BF)

        for dzl in (0, 1, 3, 2):
            for dy in (2, 1, 3, 0):
                owner = lax.rem(zl + dzl, 4) * 4 + lax.rem(y + dy, 4)
                here = k == 1 and dzl == 0 and dy == 0

                @pl.loop(0, RANKS)
                def _(i):
                    tile = fsum[k, lists[2, owner * RANKS + i]]
                    if here:
                        garr[zh, owner * RANKS + i] = tile
                    else:
                        gout[k, owner * RANKS + i] = tile

                if not here:
                    n = dzl * 4 + dy
                    to = (lax.rem(zl + dzl, 4), lax.rem(y + dy, 4), highs[k], x, c)
                    send(
                        gout.at[k, pl.ds(owner * RANKS, RANKS)], garr.at[zh, my_rows],
                        g_s.at[k, n], g_r.at[k, n], to,
                    )

    def products(half):
        phase(f"p18_dw{half}")

        @pl.loop(0, 4)
        def _(d):
            cols = pl.ds(pl.multiple_of(half * (D // 2) + d * 512, 512), 512)
            a = xs[:, :, :, cols].reshape(GROUP, 512)
            v = lax.dot_general(a, grads[...], (((0,), (0,)), ((), ())), preferred_element_type=F32)
            v = v.astype(BF).reshape(4, 2, 4, 16, 1024)
            for m in range(2):
                for xx in range(4):
                    for col in range(CPD):
                        lo = m * GROUP + col * TILE
                        for high in range(2):
                            part[m, xx, high, half, pl.ds(d * 4, 4), col] = v[:, high, xx, :, lo : lo + TILE]

        partner_send(0, half)

    products(0)
    share(0)
    y_open(0)
    partner_sum(0, 0)
    x_far(0, 0)
    x_near(0, 1, 0)
    partner_send(1, 0)
    products(1)
    y_pass(0)
    share(1)
    y_open(1)
    partner_sum(0, 1)
    x_near(0, 0, 1)
    x_far(0, 1)
    partner_send(1, 1)
    share(2)
    y_close(0)
    share(3)
    x_pass(0, 0)
    partner_sum(1, 0)
    partner_sum(1, 1)
    y_pass(1)
    y_open(2)
    x_pass(0, 1)
    for way in range(2):
        x_far(1, way)
        x_near(1, way, 1 - way)
    z_pass(0)
    y_close(1)
    y_pass(2)
    y_open(3)
    x_close(0)
    x_pass(1, 0)
    z_pass(1)
    y_close(2)
    x_pass(1, 1)
    y_pass(3)
    y_close(3)
    x_close(1)
    z_pass(2)
    z_pass(3)

    phase("p30_zrecv")
    for st in range(STAGES):
        recv(zcross.at[st], zr_s.at[st, 1], zr_r.at[st, 1])
        total = term[st, y, high_z, low_z].astype(F32) + zpair[st, high_z].astype(F32)
        total += zcross[st].astype(F32)
        dnout[:, st * COLS : (st + 1) * COLS] = total.astype(BF)

    store_dn = pltpu.make_async_copy(dnout, dn_hbm, ld.at[4])
    store_dn.start()

    for k in range(2):
        phase(f"p31_ga2a{k}")
        for n in range(16):
            if k == 1 and n == 0:
                continue
            dzl, dy = divmod(n, 4)
            src = lax.rem(zl + 4 - dzl, 4) * 4 + lax.rem(y + 4 - dy, 4)
            recv(garr.at[highs[k], pl.ds(src * RANKS, RANKS)], g_s.at[k, n], g_r.at[k, n])

    phase("p32_final")

    @pl.loop(0, OWN, unroll=4)
    def _(s):
        src = lists[3, s]
        total = garr[0, src].astype(F32) + garr[1, src].astype(F32)
        low, high = total[:8], total[8:]
        gres[c, s] = jnp.where(c == 0, low, high)
        give[s] = jnp.where(c == 0, high, low)

    phase("p33_swap")
    send(give, gres.at[c], q_s.at[0], q_r.at[0], dev(dc=1))
    store_a = pltpu.make_async_copy(gres.at[c], gt_hbm.at[c], ld.at[5])
    store_a.start()
    recv(gres.at[other], q_s.at[0], q_r.at[0])
    store_b = pltpu.make_async_copy(gres.at[other], gt_hbm.at[other], ld.at[6])
    store_b.start()
    phase("p34_drain")
    for copy in sends:
        copy.wait_send()
    for copy in (store_hid, store_dn, store_a, store_b):
        copy.wait()
    phase(None)


def hand_over(a, b, c, a_out, b_out, c_out, a_mid, b_mid, c_mid, sems):
    pairs = ((c, c_mid, c_out), (a, a_mid, a_out), (b, b_mid, b_out))
    loads = [pltpu.make_async_copy(src, mid, sems.at[i]) for i, (src, mid, _) in enumerate(pairs)]
    stores = [pltpu.make_async_copy(mid, dst, sems.at[3 + i]) for i, (_, mid, dst) in enumerate(pairs)]
    for load in loads:
        load.start()
    for load, store in zip(loads, stores):
        load.wait()
        store.start()
    for store in stores:
        store.wait()


def step(normed, cotangent, weight_tiles, slot_tile):
    dma = pltpu.SemaphoreType.DMA
    scratch = [
        pltpu.VMEM((2 * OWN, OWN), jnp.int32),
        pltpu.VMEM((8, 2 * OWN), jnp.int32),
        pltpu.SMEM((8, 2 * OWN), jnp.int32),
        pltpu.VMEM((2, OWN, 16, TILE), BF),
        pltpu.VMEM((2, 160, 16, TILE), BF),
        pltpu.VMEM((160, 16, TILE), BF),
        pltpu.VMEM((160, 16, TILE), BF),
        pltpu.VMEM((4, 4, TOK, D), BF),
        pltpu.VMEM((2, 32, 8, 16, GROUP), BF),
        pltpu.VMEM((GROUP, GROUP), BF),
        pltpu.VMEM((GROUP, GROUP), BF),
        pltpu.VMEM((2, 4, 128, GROUP), F32),
        pltpu.VMEM((GROUP, 2 * GROUP), BF),
        pltpu.VMEM((STAGES, 4, 2, 2, TOK, COLS), BF),
        pltpu.VMEM((STAGES, 2, 2, TOK, COLS), BF),
        pltpu.VMEM((STAGES, 2, 2, 2, TOK, COLS), BF),
        pltpu.VMEM((STAGES, 2, TOK, COLS), BF),
        pltpu.VMEM((STAGES, TOK, COLS), BF),
        pltpu.VMEM((TOK, D), BF),
        pltpu.VMEM((2, 4, 2, 2, 16, 4, 16, TILE), BF),
        pltpu.VMEM((4, 2, 2, 16, 4, 16, TILE), BF),
        pltpu.VMEM((2, 2, 16, 4, 16, TILE), BF),
        pltpu.VMEM((2, 2, 2, 16, 4, 16, TILE), BF),
        pltpu.VMEM((2, OWN, 16, TILE), BF),
        pltpu.VMEM((2, 160, 16, TILE), BF),
        pltpu.VMEM((2, 160, 16, TILE), BF),
        pltpu.VMEM((OWN, 8, TILE), F32),
        pltpu.VMEM((2, OWN, 8, TILE), F32),
        dma((8,)),
    ]
    for shape in (
        (len(SENT),), (3,), (4, 2, 2), (4, 2), (2, 2), (2, 2), (2, 5), (2, 4, 2), (2, 2), (2, 2, 2),
        (STAGES, 2), (STAGES, 2, 2), (STAGES, 2), (2, 16), (1,),
    ):
        scratch += [dma(shape), dma(shape)]
    anywhere = pl.BlockSpec(memory_space=pl.ANY)
    out_shape = (
        jax.ShapeDtypeStruct((GROUP, GROUP), BF),
        jax.ShapeDtypeStruct((TOK, D), BF),
        jax.ShapeDtypeStruct((2, OWN, 8, TILE), F32),
    )
    results = pl.pallas_call(
        kernel,
        out_shape=out_shape,
        in_specs=[pl.BlockSpec(memory_space=pltpu.VMEM)] + [anywhere] * 3,
        out_specs=[anywhere] * 3,
        scratch_shapes=scratch,
        compiler_params=pltpu.CompilerParams(
            collective_id=0, has_side_effects=True, vmem_limit_bytes=67_043_328
        ),
        name="gated_pair",
    )(slot_tile.reshape(OWNERS, OWN), normed, cotangent, weight_tiles)
    return pl.pallas_call(
        hand_over,
        out_shape=out_shape,
        in_specs=[anywhere] * 3,
        out_specs=[anywhere] * 3,
        scratch_shapes=[pltpu.VMEM(o.shape, o.dtype) for o in out_shape] + [dma((6,))],
        name="hand_over",
    )(*results)


def solution(mesh):
    finer = Mesh(mesh.devices.reshape(4, 4, 2, 4, 2), AXES)
    tp, dp = ("zl", "y"), ("zh", "x", "c")
    return jax.shard_map(
        step,
        mesh=finer,
        in_specs=(P(dp + tp, None), P(dp, tp), P(None, tp, None, None), P()),
        out_specs=(P(dp, tp), P(dp + tp, None), P(None, tp, dp, None)),
        check_vma=False,
    )
```

```python
import jax
import jax.numpy as jnp
from jax import lax
from jax.experimental import pallas as pl
from jax.experimental.pallas import tpu as pltpu
from jax.sharding import Mesh
from jax.sharding import PartitionSpec as P

D = 4096
FW = 8192
TILE = 128
TC = FW // TILE
OWNERS = 16
OWN = 128
CPD = TC // OWNERS
RANKS = 10
TOK = 32
GROUP = 512
AXES = ("zl", "y", "zh", "x", "c")
MESH = pl.DeviceIdType.MESH
BF = jnp.bfloat16
F32 = jnp.float32
SENT = tuple(
    [(m, dz, dy) for m in range(2) for dz in (2, 6, 1, 7, 0) for dy in range(4)
     if (dz or dy) and (dz not in (2, 6) or (dz == 2) == ((dy < 2) == (m == 0)))]
)
STAGES = 4
COLS = D // STAGES


def kernel(
    tiles_ref, tok_hbm, cot_hbm, own_hbm,
    hid_hbm, dn_hbm, gt_hbm,
    keys, rows, lists, own, outg, arrv_a, arrv_b, xs, ws, cot, hid, acc, grads, term, yfar, ynear, zpair, zcross, zdirect, dnout,
    part, precv, xfar, xnear, fsum, gout, garr, give, gres,
    ld, a_s, a_r, tz_s, tz_r, tn_s, tn_r, tf_s, tf_r, wn_s, wn_r, wf_s, wf_r, wd_s, wd_r,
    pd_s, pd_r, xf_s, xf_r, xn_s, xn_r, yf_s, yf_r, yn_s, yn_r, zr_s, zr_r, g_s, g_r, q_s, q_r,
):
    zl, y, zh, x, c = (lax.axis_index(a) for a in AXES)
    z = zh * 4 + zl
    me = zl * 4 + y
    other = 1 - c

    def dev(dz=0, dy=0, dx=0, dc=0):
        zz = lax.rem(z + dz, 8)
        return (
            lax.rem(zz, 4), lax.rem(y + dy, 4), lax.div(zz, 4), lax.rem(x + dx, 4), lax.rem(c + dc, 2),
        )

    def rcopy(src, dst, ss, rs, to):
        return pltpu.make_async_remote_copy(
            src_ref=src, dst_ref=dst, send_sem=ss, recv_sem=rs, device_id=to, device_id_type=MESH
        )

    arrv = (arrv_a, arrv_b)
    scopes = []

    def phase(name):
        if scopes:
            scopes.pop().__exit__(None, None, None)
        if name:
            scopes.append(jax.named_scope(name))
            scopes[-1].__enter__()

    sends = []

    def send(src, dst, ss, rs, to):
        copy = rcopy(src, dst, ss, rs, to)
        copy.start()
        sends.append(copy)

    def recv(dst, ss, rs):
        rcopy(dst, dst, ss, rs, dev(dc=1)).wait_recv()

    phase("p00_load")
    band = x * 2 + c
    load_own = pltpu.make_async_copy(
        own_hbm.at[:, :, pl.ds(pl.multiple_of(band * 16, 16), 16), :], own, ld.at[0]
    )
    load_tok = pltpu.make_async_copy(tok_hbm, xs.at[zl, y], ld.at[1])
    load_cot = pltpu.make_async_copy(cot_hbm, cot, ld.at[2])
    load_tok.start()
    load_own.start()

    barrier = pltpu.get_barrier_semaphore()

    @pl.loop(1, 32)
    def _(j):
        dz, dy = lax.div(j, 4), lax.rem(j, 4)
        pl.semaphore_signal(barrier, inc=1, device_id=dev(dz, dy), device_id_type=MESH)

    for to in (dev(dx=1), dev(dx=3), dev(dc=1)):
        pl.semaphore_signal(barrier, inc=1, device_id=to, device_id_type=MESH)

    phase("p01_lists")
    tiles = tiles_ref[...]
    lane = lax.broadcasted_iota(jnp.int32, (OWNERS, OWN), 1)
    owner_id = lax.broadcasted_iota(jnp.int32, (OWNERS, OWN), 0)
    target = lax.shift_right_logical(tiles & (TC - 1), 2)
    place = lax.shift_right_logical(tiles, 6) * CPD + (tiles & (TC - 1)) - me * CPD
    shift = (target & 7) * 4
    one = lax.shift_left(jnp.ones_like(tiles), shift)
    count = [jnp.where(target < 8, one, 0), jnp.where(target < 8, 0, one)]
    for step_of in (1, 2, 4, 8, 16, 32, 64):
        count = [v + jnp.where(lane >= step_of, pltpu.roll(v, step_of, 1), 0) for v in count]
    count = jnp.where(target < 8, count[0], count[1])
    rank = jnp.maximum((lax.shift_right_logical(count, shift) & 15) - 1, 0)
    mine = target == me
    last = OWNERS * RANKS - 1
    source = jnp.minimum(owner_id * RANKS + rank, last)
    code = jnp.minimum(target * RANKS + rank, last)
    my_code = jnp.max(jnp.where(owner_id == me, code, 0), axis=0, keepdims=True)
    key_a, key_b = jnp.where(mine, place, -1), jnp.where(mine, source, -1)
    codes = lax.broadcasted_iota(jnp.int32, (OWNERS * RANKS, OWN), 0)
    spot = codes[:OWN]
    inverse, gpick = jnp.zeros_like(spot), jnp.zeros_like(codes)
    for o in range(OWNERS):
        row = slice(o, o + 1)
        inverse = jnp.maximum(inverse, jnp.where(key_a[row] == spot, source[row], 0))
        gpick = jnp.maximum(gpick, jnp.where(key_b[row] == codes, place[row], 0))
    wide = lax.broadcasted_iota(jnp.int32, codes.shape, 1)
    pick = jnp.max(jnp.where(my_code == codes, wide, 0), axis=1, keepdims=True)
    inverse = jnp.max(inverse, axis=1, keepdims=True)
    gpick = jnp.max(gpick, axis=1, keepdims=True)
    columns = jnp.where(wide == 0, pick, jnp.where(wide == 2, gpick, 0))
    keys[0:OWN] = jnp.where(wide[:OWN] == 1, inverse, columns[:OWN])
    keys[OWN : OWNERS * RANKS] = columns[OWN:]
    keys[OWNERS * RANKS :] = jnp.zeros((2 * OWN - OWNERS * RANKS, OWN), jnp.int32)
    rows[:, :OWN] = keys[:OWN].T[:8]
    rows[:, OWN:] = keys[OWN:].T[:8]
    rows[3:4, :OWN] = my_code
    load_lists = pltpu.make_async_copy(rows, lists, ld.at[7])
    load_lists.start()

    load_own.wait()
    load_lists.wait()
    my_rows = pl.ds(me * RANKS, RANKS)

    def tp_of(dz, dy):
        return lax.rem(lax.rem(z + dz, 8), 4) * 4 + lax.rem(y + dy, 4)

    def pick_tiles(m):
        @pl.loop(0, OWNERS)
        def _(t):
            for k in range(RANKS):
                outg[m, t * RANKS + k] = own[m, lists[0, t * RANKS + k]]

    def send_tiles(m):
        for n, (mm, dz, dy) in enumerate(SENT):
            if mm == m:
                rows_of = pl.ds(tp_of(dz, dy) * RANKS, RANKS)
                send(outg.at[m, rows_of], arrv[m].at[my_rows], a_s.at[n], a_r.at[n], dev(dz, dy))

    phase("p02_pick0")
    pick_tiles(0)
    phase("p02_barrier")
    pl.semaphore_wait(barrier, 34)
    phase("p03_pick_send")
    send_tiles(0)
    pick_tiles(1)
    send_tiles(1)
    load_cot.start()
    load_tok.wait()

    pair = zl + 1 - 2 * lax.rem(zl, 2)
    cross = lax.rem(zl + 2, 4)

    def zq_of(q):
        return (zl, pair, cross, 3 - zl)[q]

    def at_z(to):
        return (to, y, zh, x, c)

    def near_tokens(q):
        for part_of in range(2):
            for way in range(2):
                h = way if part_of == 0 else 1 - way
                block = xs.at[zq_of(q), y, pl.ds(16 * h, 16)]
                send(block, block, tn_s.at[q, way, h], tn_r.at[q, way, h], y_to[way])

    def far_tokens(q):
        phase(f"p08_far{q}")
        for way in range(2):
            src = lax.rem(y + (3 if way == 0 else 1), 4)
            half = xs.at[zq_of(q), src, pl.ds(16 * way, 16)]
            recv(half, tn_s.at[q, way, way], tn_r.at[q, way, way])
            send(half, half, tf_s.at[q, way], tf_r.at[q, way], y_to[way])

    def last_tokens(q):
        phase(f"p14_last{q}")
        for way in range(2):
            src, h = lax.rem(y + (3 if way == 0 else 1), 4), 1 - way
            recv(xs.at[zq_of(q), src, pl.ds(16 * h, 16)], tn_s.at[q, way, h], tn_r.at[q, way, h])
            recv(xs.at[zq_of(q), lax.rem(y + 2, 4), pl.ds(16 * way, 16)], tf_s.at[q, way], tf_r.at[q, way])

    x_to = (dev(dx=1), dev(dx=3))
    y_to = (dev(dy=1), dev(dy=3))
    near_tokens(0)

    for m in range(2):
        for k in range(RANKS):
            arrv[m][me * RANKS + k] = own[m, lists[0, me * RANKS + k]]

    phase("p04_tokz")
    for i, to in enumerate((pair, cross)):
        send(xs.at[zl, y], xs.at[zl, y], tz_s.at[i], tz_r.at[i], at_z(to))

    def side_band(way, core):
        return lax.rem(x + (3 if way == 0 else 1), 4) * 2 + core

    far_x = lax.rem(x + 2, 4) * 2

    def own_weights(m):
        phase(f"p05_wait_a2a{m}")
        for n, (mm, dz, dy) in enumerate(SENT):
            if mm == m:
                t = tp_of(8 - dz, 4 - dy)
                recv(arrv[m].at[pl.ds(t * RANKS, RANKS)], a_s.at[n], a_r.at[n])
        phase(f"p06_place{m}")

        @pl.loop(0, D // TILE)
        def _(r):
            for col in range(CPD):
                ws[m, r, band, :, col * TILE : (col + 1) * TILE] = arrv[m][lists[1, r * CPD + col]]

        block = ws.at[m, :, band]
        for way in range(2):
            send(block, block, wn_s.at[m, way], wn_r.at[m, way], x_to[way])
        send(block, block, wd_s.at[m, 0], wd_r.at[m, 0], dev(dc=1))

    def near_weights(m):
        phase(f"p09_nearw{m}")
        for way in range(2):
            block = ws.at[m, :, side_band(way, c)]
            recv(block, wn_s.at[m, way], wn_r.at[m, way])
            half = ws.at[m, pl.ds(16 * way, 16), side_band(way, c)]
            send(half, half, wf_s.at[m, way], wf_r.at[m, way], x_to[way])
            send(block, block, wd_s.at[m, 1 + way], wd_r.at[m, 1 + way], dev(dc=1))

    def far_weights(m):
        phase(f"p13_farw{m}")
        for way in range(2):
            half = ws.at[m, pl.ds(16 * way, 16), far_x + c]
            recv(half, wf_s.at[m, way], wf_r.at[m, way])
            send(half, half, wd_s.at[m, 3 + way], wd_r.at[m, 3 + way], dev(dc=1))

    def partner_weights(m):
        phase(f"p15_d2d{m}")
        recv(ws.at[m, :, x * 2 + other], wd_s.at[m, 0], wd_r.at[m, 0])
        for way in range(2):
            recv(ws.at[m, :, side_band(way, other)], wd_s.at[m, 1 + way], wd_r.at[m, 1 + way])
            recv(ws.at[m, pl.ds(16 * way, 16), far_x + other], wd_s.at[m, 3 + way], wd_r.at[m, 3 + way])

    def tokens_z(q):
        phase(f"p07_tokz{q}")
        block = xs.at[zq_of(q), y]
        recv(block, tz_s.at[q - 1], tz_r.at[q - 1])
        if q == 2:
            send(block, block, tz_s.at[2], tz_r.at[2], at_z(pair))
        near_tokens(q)

    high_z, low_z = lax.div(zl, 2), lax.rem(zl, 2)

    def forward(t, matrices):
        phase(f"p16_fwd{t}{matrices[0]}")
        hh = high_z if t == 0 else 1 - high_z
        rows_of = pl.ds(pl.multiple_of(hh * (GROUP // 2), GROUP // 2), GROUP // 2)

        @pl.loop(0, 4)
        def _(k):
            cols = pl.ds(pl.multiple_of(k * 1024, 1024), 1024)
            a = xs[pl.ds(hh * 2, 2), :, :, cols].reshape(GROUP // 2, 1024)
            for m in matrices:
                w = ws[m, pl.ds(k * 8, 8)].reshape(1024, GROUP)
                v = jnp.dot(a, w, preferred_element_type=F32)

                @pl.when(k == 0)
                def _():
                    acc[m, rows_of] = v

                @pl.when(k > 0)
                def _():
                    acc[m, rows_of] += v

    own_weights(0)
    own_weights(1)
    near_weights(0)
    far_tokens(0)
    tokens_z(1)
    tokens_z(2)
    far_tokens(1)
    tokens_z(3)
    near_weights(1)
    far_tokens(2)
    far_weights(0)
    last_tokens(0)
    last_tokens(1)
    partner_weights(0)
    forward(0, (0,))
    far_tokens(3)
    far_weights(1)
    partner_weights(1)
    forward(0, (1,))
    last_tokens(2)
    last_tokens(3)
    forward(1, (0, 1))
    phase("p17_elem")
    load_cot.wait()

    @pl.loop(0, 16)
    def _(i):
        rows_of = pl.ds(pl.multiple_of(i * 32, 32), 32)
        gate, up = acc[0, rows_of], acc[1, rows_of]
        s = jax.nn.sigmoid(gate)
        act = gate * s
        ct = cot[rows_of].astype(F32)
        hid[rows_of] = (act * up).astype(BF)
        grads[rows_of, :GROUP] = (ct * up * (s * (1.0 + gate * (1.0 - s)))).astype(BF)
        grads[rows_of, GROUP:] = (ct * act).astype(BF)

    store_hid = pltpu.make_async_copy(hid, hid_hbm, ld.at[3])
    store_hid.start()

    def share(st):
        phase(f"p20_dn{st}")

        @pl.loop(0, COLS // 512)
        def _(d):
            v = None
            for m in range(2):
                w = ws[m, pl.ds(st * (COLS // TILE) + d * 4, 4)].reshape(GROUP, GROUP)
                g = grads[:, m * GROUP : (m + 1) * GROUP]
                t = lax.dot_general(g, w, (((1,), (1,)), ((), ())), preferred_element_type=F32)
                v = t if v is None else v + t
            v = v.astype(BF).reshape(2, 2, 4, TOK, 512)
            cols = pl.ds(pl.multiple_of(d * 512, 512), 512)
            for yy in range(4):
                term[st, yy, :, :, :, cols] = v[:, :, yy]

    def ring(pos):
        return lax.rem(pos + 2, 4), lax.rem(pos + 1, 4), lax.rem(pos + 3, 4), pos

    xt, yt = ring(x), ring(y)

    def ring_open(a, t, far, near, fs, fr, ss, rs, to):
        for way in range(2):
            send(a(t[0], way), far.at[way], fs.at[way], fr.at[way], to[way])
        for way in range(2):
            h = 1 - way
            send(a(t[1 + way], h), near.at[way, h], ss.at[way, h], rs.at[way, h], to[way])

    def ring_pass(a, t, far, near, fs, fr, ss, rs, to, add):
        for way in range(2):
            recv(far.at[way], fs.at[way], fr.at[way])
            add(t[1 + way], way)
            send(a(t[1 + way], way), near.at[way, way], ss.at[way, way], rs.at[way, way], to[way])

    def ring_close(near, ss, rs):
        for way in range(2):
            for h in range(2):
                recv(near.at[way, h], ss.at[way, h], rs.at[way, h])

    def y_args(st):
        a = lambda t, h: term.at[st, t, h]
        return a, yt, yfar.at[st], ynear.at[st], yf_s.at[st], yf_r.at[st], yn_s.at[st], yn_r.at[st], y_to

    def y_open(st):
        ring_open(*y_args(st))

    def y_pass(st):
        phase(f"p23_ypass{st}")

        def add(t, way):
            here = term[st, t, way].astype(F32)
            term[st, t, way] = (here + yfar[st, way].astype(F32)).astype(BF)

        ring_pass(*y_args(st), add)

    def y_close(st):
        phase(f"p25_yclose{st}")
        ring_close(ynear.at[st], yn_s.at[st], yn_r.at[st])
        for h in range(2):
            total = term[st, y, h].astype(F32)
            for way in range(2):
                total += ynear[st, way, h].astype(F32)
            term[st, y, h] = total.astype(BF)
        if st < 2:
            send(
                term.at[st, y, :, lax.rem(pair, 2)], zpair.at[st], zr_s.at[st, 0], zr_r.at[st, 0], at_z(pair)
            )
            return
        for j in range(1, 4):
            zt = lax.rem(zl + j, 4)
            send(
                term.at[st, y, lax.div(zt, 2), lax.rem(zt, 2)], zdirect.at[st - 2, j - 1],
                zr_s.at[st, j - 1], zr_r.at[st, j - 1], at_z(zt),
            )

    def z_pass(st):
        phase(f"p26_zpass{st}")
        recv(zpair.at[st], zr_s.at[st, 0], zr_r.at[st, 0])
        here = term[st, y, 1 - high_z, low_z].astype(F32)
        term[st, y, 1 - high_z, low_z] = (here + zpair[st, 1 - high_z].astype(F32)).astype(BF)
        send(
            term.at[st, y, 1 - high_z, low_z], zcross.at[st], zr_s.at[st, 1], zr_r.at[st, 1], at_z(cross)
        )

    highs = (1 - zh, zh)
    mat = part.at[c]

    def pieces(h):
        return (0, 2 - h, 1 + h, 3)

    def partner_send(k, h):
        for i in pieces(h):
            send(
                part.at[other, xt[i], highs[k], h], precv.at[xt[i], highs[k], h],
                pd_s.at[k, i, h], pd_r.at[k, i, h], dev(dc=1),
            )

    def partner_sum(k, h):
        phase(f"p22_partner{k}{h}")
        for n, i in enumerate(pieces(h)):
            recv(precv.at[xt[i], highs[k], h], pd_s.at[k, i, h], pd_r.at[k, i, h])

            @pl.loop(0, 4)
            def _(r):
                at = (xt[i], highs[k], h, pl.ds(r * 4, 4))
                mat[at] = (mat[at].astype(F32) + precv[at].astype(F32)).astype(BF)

            if k == 0 and n == 0:
                x_far(0, h)
            if k == 0 and n == 1:
                x_near(0, 1 - h, h)

    def x_far(k, way):
        send(mat.at[xt[0], highs[k], way], xfar.at[k, way], xf_s.at[k, way], xf_r.at[k, way], x_to[way])

    def x_near(k, way, h):
        send(
            mat.at[xt[1 + way], highs[k], h], xnear.at[k, way, h], xn_s.at[k, way, h], xn_r.at[k, way, h],
            x_to[way],
        )

    def x_pass(k, way):
        phase(f"p24_xpass{k}{way}")
        recv(xfar.at[k, way], xf_s.at[k, way], xf_r.at[k, way])

        @pl.loop(0, 4)
        def _(r):
            rs = pl.ds(r * 4, 4)
            at = (xt[1 + way], highs[k], way, rs)
            mat[at] = (mat[at].astype(F32) + xfar[k, way, rs].astype(F32)).astype(BF)

        x_near(k, way, way)

    def x_close(k):
        phase(f"p27_xclose{k}")
        ring_close(xnear.at[k], xn_s.at[k], xn_r.at[k])
        for h in range(2):

            @pl.loop(0, 16)
            def _(r):
                total = mat[x, highs[k], h, r].astype(F32)
                for way in range(2):
                    total += xnear[k, way, h, r].astype(F32)
                fsum[k, pl.ds((h * 16 + r) * CPD, CPD)] = total.astype(BF)

        for dzl in (0, 1, 3, 2):
            for dy in (2, 1, 3, 0):
                owner = lax.rem(zl + dzl, 4) * 4 + lax.rem(y + dy, 4)
                here = k == 1 and dzl == 0 and dy == 0

                @pl.loop(0, RANKS)
                def _(i):
                    tile = fsum[k, lists[2, owner * RANKS + i]]
                    if here:
                        garr[zh, owner * RANKS + i] = tile
                    else:
                        gout[k, owner * RANKS + i] = tile

                if not here:
                    n = dzl * 4 + dy
                    to = (lax.rem(zl + dzl, 4), lax.rem(y + dy, 4), highs[k], x, c)
                    send(
                        gout.at[k, pl.ds(owner * RANKS, RANKS)], garr.at[zh, my_rows],
                        g_s.at[k, n], g_r.at[k, n], to,
                    )

    def products(half):
        phase(f"p18_dw{half}")

        @pl.loop(0, 4)
        def _(d):
            cols = pl.ds(pl.multiple_of(half * (D // 2) + d * 512, 512), 512)
            a = xs[:, :, :, cols].reshape(GROUP, 512)
            v = lax.dot_general(a, grads[...], (((0,), (0,)), ((), ())), preferred_element_type=F32)
            v = v.astype(BF).reshape(4, 2, 4, 16, 1024)
            for m in range(2):
                for xx in range(4):
                    for col in range(CPD):
                        lo = m * GROUP + col * TILE
                        for high in range(2):
                            part[m, xx, high, half, pl.ds(d * 4, 4), col] = v[:, high, xx, :, lo : lo + TILE]

        partner_send(0, half)

    products(0)
    share(0)
    y_open(0)
    partner_sum(0, 0)
    partner_send(1, 0)
    products(1)
    share(1)
    partner_sum(0, 1)
    partner_send(1, 1)
    y_pass(0)
    y_open(1)
    share(2)
    y_close(0)
    share(3)
    x_pass(0, 0)
    partner_sum(1, 0)
    partner_sum(1, 1)
    y_pass(1)
    y_open(2)
    x_pass(0, 1)
    for way in range(2):
        x_far(1, way)
        x_near(1, way, 1 - way)
    z_pass(0)
    y_close(1)
    x_close(0)
    y_pass(2)
    y_open(3)
    x_pass(1, 0)
    z_pass(1)
    y_close(2)
    x_pass(1, 1)
    y_pass(3)
    x_close(1)
    y_close(3)

    phase("p30_zrecv")
    for st in range(STAGES):
        total = term[st, y, high_z, low_z].astype(F32)
        if st < 2:
            recv(zcross.at[st], zr_s.at[st, 1], zr_r.at[st, 1])
            total += zpair[st, high_z].astype(F32)
            total += zcross[st].astype(F32)
        else:
            for j in range(3):
                recv(zdirect.at[st - 2, j], zr_s.at[st, j], zr_r.at[st, j])
                total += zdirect[st - 2, j].astype(F32)
        dnout[:, st * COLS : (st + 1) * COLS] = total.astype(BF)

    store_dn = pltpu.make_async_copy(dnout, dn_hbm, ld.at[4])
    store_dn.start()

    for k in range(2):
        phase(f"p31_ga2a{k}")
        for n in range(16):
            if k == 1 and n == 0:
                continue
            dzl, dy = divmod(n, 4)
            src = lax.rem(zl + 4 - dzl, 4) * 4 + lax.rem(y + 4 - dy, 4)
            recv(garr.at[highs[k], pl.ds(src * RANKS, RANKS)], g_s.at[k, n], g_r.at[k, n])

    phase("p32_final")

    @pl.loop(0, OWN, unroll=4)
    def _(s):
        src = lists[3, s]
        total = garr[0, src].astype(F32) + garr[1, src].astype(F32)
        low, high = total[:8], total[8:]
        gres[c, s] = jnp.where(c == 0, low, high)
        give[s] = jnp.where(c == 0, high, low)

    phase("p33_swap")
    send(give, gres.at[c], q_s.at[0], q_r.at[0], dev(dc=1))
    store_a = pltpu.make_async_copy(gres.at[c], gt_hbm.at[c], ld.at[5])
    store_a.start()
    recv(gres.at[other], q_s.at[0], q_r.at[0])
    store_b = pltpu.make_async_copy(gres.at[other], gt_hbm.at[other], ld.at[6])
    store_b.start()
    phase("p34_drain")
    for copy in sends:
        copy.wait_send()
    for copy in (store_hid, store_dn, store_a, store_b):
        copy.wait()
    phase(None)


def hand_over(a, b, c, a_out, b_out, c_out, a_mid, b_mid, c_mid, sems):
    pairs = ((c, c_mid, c_out), (a, a_mid, a_out), (b, b_mid, b_out))
    loads = [pltpu.make_async_copy(src, mid, sems.at[i]) for i, (src, mid, _) in enumerate(pairs)]
    stores = [pltpu.make_async_copy(mid, dst, sems.at[3 + i]) for i, (_, mid, dst) in enumerate(pairs)]
    for load in loads:
        load.start()
    for load, store in zip(loads, stores):
        load.wait()
        store.start()
    for store in stores:
        store.wait()


def step(normed, cotangent, weight_tiles, slot_tile):
    dma = pltpu.SemaphoreType.DMA
    scratch = [
        pltpu.VMEM((2 * OWN, OWN), jnp.int32),
        pltpu.VMEM((8, 2 * OWN), jnp.int32),
        pltpu.SMEM((8, 2 * OWN), jnp.int32),
        pltpu.VMEM((2, OWN, 16, TILE), BF),
        pltpu.VMEM((2, 160, 16, TILE), BF),
        pltpu.VMEM((160, 16, TILE), BF),
        pltpu.VMEM((160, 16, TILE), BF),
        pltpu.VMEM((4, 4, TOK, D), BF),
        pltpu.VMEM((2, 32, 8, 16, GROUP), BF),
        pltpu.VMEM((GROUP, GROUP), BF),
        pltpu.VMEM((GROUP, GROUP), BF),
        pltpu.VMEM((2, GROUP, GROUP), F32),
        pltpu.VMEM((GROUP, 2 * GROUP), BF),
        pltpu.VMEM((STAGES, 4, 2, 2, TOK, COLS), BF),
        pltpu.VMEM((STAGES, 2, 2, TOK, COLS), BF),
        pltpu.VMEM((STAGES, 2, 2, 2, TOK, COLS), BF),
        pltpu.VMEM((2, 2, TOK, COLS), BF),
        pltpu.VMEM((2, TOK, COLS), BF),
        pltpu.VMEM((2, 3, TOK, COLS), BF),
        pltpu.VMEM((TOK, D), BF),
        pltpu.VMEM((2, 4, 2, 2, 16, 4, 16, TILE), BF),
        pltpu.VMEM((4, 2, 2, 16, 4, 16, TILE), BF),
        pltpu.VMEM((2, 2, 16, 4, 16, TILE), BF),
        pltpu.VMEM((2, 2, 2, 16, 4, 16, TILE), BF),
        pltpu.VMEM((2, OWN, 16, TILE), BF),
        pltpu.VMEM((2, 160, 16, TILE), BF),
        pltpu.VMEM((2, 160, 16, TILE), BF),
        pltpu.VMEM((OWN, 8, TILE), F32),
        pltpu.VMEM((2, OWN, 8, TILE), F32),
        dma((8,)),
    ]
    for shape in (
        (len(SENT),), (3,), (4, 2, 2), (4, 2), (2, 2), (2, 2), (2, 5), (2, 4, 2), (2, 2), (2, 2, 2),
        (STAGES, 2), (STAGES, 2, 2), (STAGES, 3), (2, 16), (1,),
    ):
        scratch += [dma(shape), dma(shape)]
    anywhere = pl.BlockSpec(memory_space=pl.ANY)
    out_shape = (
        jax.ShapeDtypeStruct((GROUP, GROUP), BF),
        jax.ShapeDtypeStruct((TOK, D), BF),
        jax.ShapeDtypeStruct((2, OWN, 8, TILE), F32),
    )
    results = pl.pallas_call(
        kernel,
        out_shape=out_shape,
        in_specs=[pl.BlockSpec(memory_space=pltpu.VMEM)] + [anywhere] * 3,
        out_specs=[anywhere] * 3,
        scratch_shapes=scratch,
        compiler_params=pltpu.CompilerParams(
            collective_id=0, has_side_effects=True, vmem_limit_bytes=67_043_328
        ),
        name="gated_pair",
    )(slot_tile.reshape(OWNERS, OWN), normed, cotangent, weight_tiles)
    return pl.pallas_call(
        hand_over,
        out_shape=out_shape,
        in_specs=[anywhere] * 3,
        out_specs=[anywhere] * 3,
        scratch_shapes=[pltpu.VMEM(o.shape, o.dtype) for o in out_shape] + [dma((6,))],
        name="hand_over",
    )(*results)


def solution(mesh):
    finer = Mesh(mesh.devices.reshape(4, 4, 2, 4, 2), AXES)
    tp, dp = ("zl", "y"), ("zh", "x", "c")
    return jax.shard_map(
        step,
        mesh=finer,
        in_specs=(P(dp + tp, None), P(dp, tp), P(None, tp, None, None), P()),
        out_specs=(P(dp, tp), P(dp + tp, None), P(None, tp, dp, None)),
        check_vma=False,
    )
```
